32 devices in a mesh: dp: 4 (over x, core), seq: 2 (over y), tensor: 4 (over z).
Axes of the slice: x: 2, y: 2, z: 4, core: 2. Of those that a mesh axis runs over, the one named last changes fastest.
Arguments:
- inputs: bfloat16 [4, 2, 1024, 1536], P('dp', None, 'seq'), may hold values from -6 to 6
- segment_ids: int32 [4, 2, 1024], P('dp'), may hold values from 0 to 6, as said below
- ancestry: int32 [4, 2, 7, 7], P('dp'), may hold values from 0 to 1, as said below
- w_query: bfloat16 [1536, 1536], P(None, 'tensor'), may hold values from -0.15625 to 0.15625
- key_weight: bfloat16 [1536, 768], P(None, 'tensor'), may hold values from -0.15625 to 0.15625
- value_weight: bfloat16 [1536, 768], P(None, 'tensor'), may hold values from -0.15625 to 0.15625
- w_output: bfloat16 [1536, 1536], P('tensor'), may hold values from -0.875 to 0.875
- w_gate: bfloat16 [1536, 4096], P(None, 'tensor'), may hold values from -0.15625 to 0.15625
- w_up: bfloat16 [1536, 4096], P(None, 'tensor'), may hold values from -0.15625 to 0.15625
- w_down: bfloat16 [4096, 1536], P('tensor'), may hold values from -0.09375 to 0.09375
- attn_gain: float32 [1536], replicated, may hold values from 0.5 to 1.5
- ffn_gain: float32 [1536], replicated, may hold values from 0.5 to 1.5
- cotangent: bfloat16 [4, 2, 1024, 1536], P('dp', None, 'seq'), may hold values from -6 to 6
- mom_query: float32 [1536, 1536], P(('dp', 'seq'), 'tensor'), may hold values from -12 to 12
- key_momentum: float32 [1536, 768], P(('dp', 'seq'), 'tensor'), may hold values from -12 to 12
- value_momentum: float32 [1536, 768], P(('dp', 'seq'), 'tensor'), may hold values from -12 to 12
- mom_output: float32 [1536, 1536], P('tensor', ('dp', 'seq')), may hold values from -12 to 12
- mom_gate: float32 [1536, 4096], P(('dp', 'seq'), 'tensor'), may hold values from -12 to 12
- mom_up: float32 [1536, 4096], P(('dp', 'seq'), 'tensor'), may hold values from -12 to 12
- mom_down: float32 [4096, 1536], P('tensor', ('dp', 'seq')), may hold values from -12 to 12
- attn_first: float32 [1536], replicated, may hold values from -30 to 30
- attn_second: float32 [1536], replicated, may hold values from 50 to 500
- ffn_first: float32 [1536], replicated, may hold values from -30 to 30
- ffn_second: float32 [1536], replicated, may hold values from 50 to 500
Outputs:
- block_out: float32 [4, 2, 1024, 1536], P('dp', None, 'seq')
- input_grad: float32 [4, 2, 1024, 1536], P('dp', None, 'seq')
- grad_query: float32 [1536, 1536], P(('dp', 'seq'), 'tensor')
- grad_key: float32 [1536, 768], P(('dp', 'seq'), 'tensor')
- grad_value: float32 [1536, 768], P(('dp', 'seq'), 'tensor')
- grad_output: float32 [1536, 1536], P('tensor', ('dp', 'seq'))
- grad_gate: float32 [1536, 4096], P(('dp', 'seq'), 'tensor')
- grad_up: float32 [1536, 4096], P(('dp', 'seq'), 'tensor')
- grad_down: float32 [4096, 1536], P('tensor', ('dp', 'seq'))
- attn_gain_grad: float32 [1536], replicated
- ffn_gain_grad: float32 [1536], replicated
- new_mom_query: float32 [1536, 1536], P(('dp', 'seq'), 'tensor')
- new_mom_key: float32 [1536, 768], P(('dp', 'seq'), 'tensor')
- new_mom_value: float32 [1536, 768], P(('dp', 'seq'), 'tensor')
- new_mom_output: float32 [1536, 1536], P('tensor', ('dp', 'seq'))
- new_mom_gate: float32 [1536, 4096], P(('dp', 'seq'), 'tensor')
- new_mom_up: float32 [1536, 4096], P(('dp', 'seq'), 'tensor')
- new_mom_down: float32 [4096, 1536], P('tensor', ('dp', 'seq'))
- step_query: float32 [1536, 1536], P(('dp', 'seq'), 'tensor')
- step_key: float32 [1536, 768], P(('dp', 'seq'), 'tensor')
- step_value: float32 [1536, 768], P(('dp', 'seq'), 'tensor')
- step_output: float32 [1536, 1536], P('tensor', ('dp', 'seq'))
- step_gate: float32 [1536, 4096], P(('dp', 'seq'), 'tensor')
- step_up: float32 [1536, 4096], P(('dp', 'seq'), 'tensor')
- step_down: float32 [4096, 1536], P('tensor', ('dp', 'seq'))
- attn_first_new: float32 [1536], replicated
- attn_second_new: float32 [1536], replicated
- attn_gain_step: float32 [1536], replicated
- ffn_first_new: float32 [1536], replicated
- ffn_second_new: float32 [1536], replicated
- ffn_gain_step: float32 [1536], replicated
The draws below stay inside these ranges and needn't reach their ends.
Inputs may be any that keep to these rules, and one draw needn't show every extreme that they name: `segment_ids`: in every tree: a trunk segment of 512 tokens comes first; two branch segments of 128 tokens hang from it and two leaf segments of 64 tokens from each branch; every segment lies in one run of positions after all of its ancestors; the 7 labels are distinct and their assignment varies. ancestry[., ., a, b] is 1 where segment b is segment a or one of its ancestors in that tree, else 0.
All inputs are finite; a program needn't handle non-finite values.
Results may differ from the reference program's by a relative error of at most 0.023.
Values may be sent and summed in bfloat16 or wider, within the bound.
A program may use at most 256 MiB of HBM per device.

```python
import math
import jax
import jax.numpy as jnp
import numpy as np
from jax import lax

MODEL_WIDTH = 1536
HQ = 16
SHARED_KV_HEADS = 8
HEAD_SIZE = 96
FF = 4096
TREE = 1024
SEGS = 7
MB = 2
ITERS_NS = 3
ADAM_STEP = 10
N_DP = 4
N_TENSOR = 4


ANCESTOR_TABLE = np.array([[1, 0, 0, 0, 0, 0, 0], [1, 1, 0, 0, 0, 0, 0], [1, 0, 1, 0, 0, 0, 0], [1, 1, 0, 1, 0, 0, 0], [1, 1, 0, 0, 1, 0, 0], [1, 0, 1, 0, 0, 1, 0], [1, 0, 1, 0, 0, 0, 1]], dtype=np.int32)


def tree_layout(key):
    choose = jax.random.randint(jax.random.fold_in(key, 7), (4,), 0, 2)
    labels = jax.random.permutation(jax.random.fold_in(key, 11), 7).astype(jnp.int32)
    first = 1 + choose[0]
    second = 3 - first
    first_one = 2 * first + 1 + choose[1]
    first_two = 2 * first + 2 - choose[1]
    second_one = 2 * second + 1 + choose[2]
    second_two = 2 * second + 2 - choose[2]
    anchor = jnp.zeros((), jnp.int32)
    depth_order = jnp.stack([anchor, first, first_one, first_two, second, second_one, second_two])
    width_order = jnp.stack([anchor, first, second, first_one, first_two, second_one, second_two])
    order = jnp.where(choose[3] == 1, width_order, depth_order).astype(jnp.int32)
    sizes = jnp.array([TREE // 2, TREE // 8, TREE // 8, TREE // 16, TREE // 16, TREE // 16, TREE // 16], dtype=jnp.int32)
    ends = jnp.cumsum(sizes[order])
    place = jnp.arange(TREE, dtype=jnp.int32)
    slot = jnp.sum((place[:, None] >= ends[None, :]).astype(jnp.int32), axis=1)
    seg = labels[order[slot]]
    inverse = jnp.argsort(labels)
    table = jnp.asarray(ANCESTOR_TABLE)
    anc = table[inverse][:, inverse]
    return (seg, anc)


def all_trees(key):

    def one_tree(index):
        return tree_layout(jax.random.fold_in(key, 1000 + index))
    return jax.vmap(one_tree)(jnp.arange(N_DP * MB, dtype=jnp.int32))


def draw_segment_ids(key, part):
    seg, anc = all_trees(key)
    return seg.reshape(N_DP, MB, TREE)


def draw_ancestry(key, part):
    seg, anc = all_trees(key)
    return anc.reshape(N_DP, MB, SEGS, SEGS)


def shard_levels(stream_key, extent, split, low, high):
    def one(dim, shards_of):
        steps = jax.random.uniform(jax.random.fold_in(jax.random.fold_in(stream_key, 6), dim), (shards_of,), jnp.float32, low / len(split), high / len(split))
        return jnp.repeat(jnp.exp(steps), extent[dim] // shards_of).reshape((-1,) + (1,) * (len(extent) - dim - 1))

    gain = one(*split[0])
    for cut in split[1:]:
        gain = gain * one(*cut)
    return gain


def normal_values(own_key, shape, width, limit, split=(), kind=jnp.bfloat16):
    drawn = width * jax.random.normal(own_key, shape, jnp.float32)
    if split:
        drawn = drawn * shard_levels(own_key, shape, split, -0.22, 0.18)
    return jnp.clip(drawn, -limit, limit).astype(kind)


def setup_inputs(seed: int = 0) -> dict:
    key_of = jax.random.split(jax.random.key(seed), 25)
    return {
        "inputs": normal_values(key_of[0], (N_DP, MB, TREE, MODEL_WIDTH), 1.0, 6.0, ((0, 4), (2, 2))),
        "segment_ids": draw_segment_ids(jax.random.fold_in(key_of[24], 71), 0),
        "ancestry": draw_ancestry(jax.random.fold_in(key_of[24], 71), 0),
        "w_query": normal_values(key_of[3], (MODEL_WIDTH, HQ * HEAD_SIZE), MODEL_WIDTH ** -0.5, 0.15625, ((1, 4),)),
        "key_weight": normal_values(key_of[4], (MODEL_WIDTH, SHARED_KV_HEADS * HEAD_SIZE), MODEL_WIDTH ** -0.5, 0.15625, ((1, 4),)),
        "value_weight": normal_values(key_of[5], (MODEL_WIDTH, SHARED_KV_HEADS * HEAD_SIZE), MODEL_WIDTH ** -0.5, 0.15625, ((1, 4),)),
        "w_output": normal_values(key_of[6], (HQ * HEAD_SIZE, MODEL_WIDTH), (HQ * HEAD_SIZE // 32) ** -0.5, 0.875, ((0, 4),)),
        "w_gate": normal_values(key_of[7], (MODEL_WIDTH, FF), MODEL_WIDTH ** -0.5, 0.15625, ((1, 4),)),
        "w_up": normal_values(key_of[8], (MODEL_WIDTH, FF), MODEL_WIDTH ** -0.5, 0.15625, ((1, 4),)),
        "w_down": normal_values(key_of[9], (FF, MODEL_WIDTH), FF ** -0.5, 0.09375, ((0, 4),)),
        "attn_gain": jnp.clip(1.0 + 0.1 * jax.random.normal(key_of[10], (MODEL_WIDTH,), jnp.float32), 0.5, 1.5),
        "ffn_gain": jnp.clip(1.0 + 0.1 * jax.random.normal(key_of[11], (MODEL_WIDTH,), jnp.float32), 0.5, 1.5),
        "cotangent": normal_values(key_of[12], (N_DP, MB, TREE, MODEL_WIDTH), 1.0, 6.0, ((0, 4), (2, 2))),
        "mom_query": normal_values(key_of[13], (MODEL_WIDTH, HQ * HEAD_SIZE), 2.0, 12.0, ((0, 8), (1, 4)), jnp.float32),
        "key_momentum": normal_values(key_of[14], (MODEL_WIDTH, SHARED_KV_HEADS * HEAD_SIZE), 2.0, 12.0, ((0, 8), (1, 4)), jnp.float32),
        "value_momentum": normal_values(key_of[15], (MODEL_WIDTH, SHARED_KV_HEADS * HEAD_SIZE), 2.0, 12.0, ((0, 8), (1, 4)), jnp.float32),
        "mom_output": normal_values(key_of[16], (HQ * HEAD_SIZE, MODEL_WIDTH), 2.0, 12.0, ((0, 4), (1, 8)), jnp.float32),
        "mom_gate": normal_values(key_of[17], (MODEL_WIDTH, FF), 2.0, 12.0, ((0, 8), (1, 4)), jnp.float32),
        "mom_up": normal_values(key_of[18], (MODEL_WIDTH, FF), 2.0, 12.0, ((0, 8), (1, 4)), jnp.float32),
        "mom_down": normal_values(key_of[19], (FF, MODEL_WIDTH), 2.0, 12.0, ((0, 4), (1, 8)), jnp.float32),
        "attn_first": normal_values(key_of[20], (MODEL_WIDTH,), 5.0, 30.0, (), jnp.float32),
        "attn_second": jnp.clip(jnp.exp(jax.random.uniform(key_of[21], (MODEL_WIDTH,), jnp.float32, math.log(50.0), math.log(500.0))), 50.0, 500.0),
        "ffn_first": normal_values(key_of[22], (MODEL_WIDTH,), 5.0, 30.0, (), jnp.float32),
        "ffn_second": jnp.clip(jnp.exp(jax.random.uniform(key_of[23], (MODEL_WIDTH,), jnp.float32, math.log(50.0), math.log(500.0))), 50.0, 500.0),
    }


@jax.custom_vjp
def low(v):
    return lax.optimization_barrier(v.astype(jnp.bfloat16)).astype(jnp.float32)

@jax.custom_vjp
def low_back(v):
    return v

def low_keep(v):
    return (low(v), None)

def low_pass(kept, grad):
    return (grad,)

def back_keep(v):
    return (v, None)

def back_low(kept, grad):
    return (low(grad),)
low.defvjp(low_keep, low_pass)
low_back.defvjp(back_keep, back_low)
HIGH = lax.Precision.HIGHEST
EPS_NORM = 1e-05
ROPE_THETA = 100000.0
MU_MUON = 0.95
NS_A = 3.4445
NS_B = -4.775
NS_C = 2.0315
LR_MUON = 0.1
EPS_MUON = 1e-07
BETA_ONE = 0.9
BETA_TWO = 0.95
LR_ADAM = 0.01
EPS_ADAM = 1e-08

def rms_scale(values):
    return lax.rsqrt(lax.optimization_barrier(jnp.mean(values * values, axis=-1, keepdims=True)) + EPS_NORM)

def rotary_tables(positions):
    half = HEAD_SIZE // 2
    freq = jnp.power(ROPE_THETA, -(2.0 * jnp.arange(half, dtype=jnp.float32)) / HEAD_SIZE)
    angle = positions[..., None] * freq
    return (jnp.cos(angle), jnp.sin(angle))

def rotary(values, cosine, sine):
    shape = values.shape
    heads = values.reshape(shape[:-1] + (shape[-1] // HEAD_SIZE, HEAD_SIZE))
    half = HEAD_SIZE // 2
    front = heads[..., :half]
    back = heads[..., half:]
    cos_h = cosine[..., None, :]
    sin_h = sine[..., None, :]
    return jnp.concatenate([front * cos_h - back * sin_h, back * cos_h + front * sin_h], axis=-1).reshape(shape)

def attend(packed):
    query, key, value, allowed = packed
    kv_heads = key.shape[-1] // HEAD_SIZE
    group = query.shape[-1] // key.shape[-1]
    query_heads = query.reshape(TREE, kv_heads, group, HEAD_SIZE)
    key_heads = key.reshape(TREE, kv_heads, HEAD_SIZE)
    value_heads = value.reshape(TREE, kv_heads, HEAD_SIZE)
    scores = jnp.einsum('tkgd,skd->kgts', query_heads, key_heads, precision=HIGH) * (1.0 / math.sqrt(HEAD_SIZE))
    scores = low_back(scores)
    masked = jnp.where(allowed[None, None], scores, -1e+30)
    probs = low(jax.nn.softmax(masked, axis=-1))
    mixed = jnp.einsum('kgts,skd->tkgd', probs, value_heads, precision=HIGH)
    return mixed.reshape(TREE, query.shape[-1])

def path_of(table, ids):
    return table[ids[:, None], ids[None, :]]

def muon(grad, mom, flip):
    moment = MU_MUON * mom + grad
    work = moment.T if flip else moment
    cols = work.shape[1] // N_TENSOR
    blocks = work.reshape(MODEL_WIDTH, N_TENSOR, cols).transpose(1, 0, 2)
    norm = jnp.sqrt(lax.optimization_barrier(jnp.sum(blocks * blocks, axis=(1, 2), keepdims=True)))
    ortho = blocks / (norm + EPS_MUON)
    for turn in range(ITERS_NS):
        gram = jnp.einsum('nlc,nle->nce', ortho, ortho, precision=HIGH)
        poly = NS_B * gram + NS_C * jnp.einsum('nce,nef->ncf', gram, gram, precision=HIGH)
        ortho = NS_A * ortho + jnp.einsum('nlc,nce->nle', ortho, poly, precision=HIGH)
    update = -LR_MUON * 0.2 * math.sqrt(MODEL_WIDTH) * ortho.transpose(1, 0, 2).reshape(MODEL_WIDTH, N_TENSOR * cols)
    if flip:
        update = update.T
    return (moment, update)

def adam(grad, first, second):
    first_new = BETA_ONE * first + (1.0 - BETA_ONE) * grad
    second_new = BETA_TWO * second + (1.0 - BETA_TWO) * grad * grad
    corrected = first_new / (1.0 - BETA_ONE ** ADAM_STEP)
    spread = jnp.sqrt(second_new / (1.0 - BETA_TWO ** ADAM_STEP)) + EPS_ADAM
    return (first_new, second_new, -LR_ADAM * corrected / spread)

def reference(inputs, segment_ids, ancestry, w_query, key_weight, value_weight, w_output, w_gate, w_up, w_down, attn_gain, ffn_gain, cotangent, mom_query, key_momentum, value_momentum, mom_output, mom_gate, mom_up, mom_down, attn_first, attn_second, ffn_first, ffn_second):
    trees = N_DP * MB
    flat_in = inputs.reshape(trees, TREE, MODEL_WIDTH).astype(jnp.float32)
    seg = segment_ids.reshape(trees, TREE)
    anc = ancestry.reshape(trees, SEGS, SEGS)
    on_path = jax.vmap(path_of)(anc, seg) == 1
    place = jnp.arange(TREE, dtype=jnp.int32)
    allowed = on_path & (place[:, None] >= place[None, :])[None]
    positions = (lax.optimization_barrier(jnp.sum(allowed.astype(jnp.int32), axis=2)) - 1).astype(jnp.float32)
    cosine, sine = rotary_tables(positions)

    def layer(resid, wq, wk, wv, wo, wg, wu, wd, gain_one, gain_two):
        normed = low(resid * rms_scale(resid) * gain_one)
        query = low(rotary(low_back(jnp.einsum('ntd,de->nte', normed, wq, precision=HIGH)), cosine, sine))
        key = low(rotary(low_back(jnp.einsum('ntd,de->nte', normed, wk, precision=HIGH)), cosine, sine))
        value = low(low_back(jnp.einsum('ntd,de->nte', normed, wv, precision=HIGH)))
        mixed = lax.map(jax.checkpoint(attend), (query, key, value, allowed))
        mixed = low_back(low(mixed))
        attn = low_back(jnp.einsum('nte,ed->ntd', mixed, wo, precision=HIGH))
        middle = resid + attn
        normed_two = low(middle * rms_scale(middle) * gain_two)
        gate = low_back(jnp.einsum('ntd,df->ntf', normed_two, wg, precision=HIGH))
        up_value = low_back(jnp.einsum('ntd,df->ntf', normed_two, wu, precision=HIGH))
        inner = low(jax.nn.silu(gate) * up_value)
        return middle + jnp.einsum('ntf,fd->ntd', inner, wd, precision=HIGH)
    block_out, pullback = jax.vjp(layer, flat_in, w_query.astype(jnp.float32), key_weight.astype(jnp.float32), value_weight.astype(jnp.float32), w_output.astype(jnp.float32), w_gate.astype(jnp.float32), w_up.astype(jnp.float32), w_down.astype(jnp.float32), attn_gain, ffn_gain)
    grads = pullback(cotangent.reshape(trees, TREE, MODEL_WIDTH).astype(jnp.float32))
    new_q, step_q = muon(grads[1], mom_query, False)
    new_k, step_k = muon(grads[2], key_momentum, False)
    new_v, step_v = muon(grads[3], value_momentum, False)
    new_o, step_o = muon(grads[4], mom_output, True)
    new_g, step_g = muon(grads[5], mom_gate, False)
    new_u, step_u = muon(grads[6], mom_up, False)
    new_d, step_d = muon(grads[7], mom_down, True)
    attn_one, attn_two, attn_step = adam(grads[8], attn_first, attn_second)
    ffn_one, ffn_two, ffn_step = adam(grads[9], ffn_first, ffn_second)
    shape = (N_DP, MB, TREE, MODEL_WIDTH)
    return (block_out.reshape(shape), grads[0].reshape(shape), grads[1], grads[2], grads[3], grads[4], grads[5], grads[6], grads[7], grads[8], grads[9], new_q, new_k, new_v, new_o, new_g, new_u, new_d, step_q, step_k, step_v, step_o, step_g, step_u, step_d, attn_one, attn_two, attn_step, ffn_one, ffn_two, ffn_step)
```

```python
import functools
import math

import jax
import jax.numpy as jnp
from jax import lax
from jax.experimental import pallas as pl
from jax.experimental.pallas import tpu as pltpu
from jax.sharding import PartitionSpec as P

MODEL_WIDTH = 1536
HEAD_SIZE = 96
ITERS_NS = 3
ADAM_STEP = 10


EPS_NORM = 1e-05
ROPE_THETA = 100000.0
MU_MUON = 0.95
NS_A = 3.4445
NS_B = -4.775
NS_C = 2.0315
LR_MUON = 0.1
EPS_MUON = 1e-07
BETA_ONE = 0.9
BETA_TWO = 0.95
LR_ADAM = 0.01
EPS_ADAM = 1e-08
LOW = jnp.bfloat16
F32 = jnp.float32


def rms_scale(values):
    return lax.rsqrt(jnp.mean(values * values, axis=-1, keepdims=True) + EPS_NORM)


def norm_back(upstream, plain, scale, gain):
    scaled = upstream * gain
    return scale * (scaled - plain * jnp.mean(scaled * plain, axis=-1, keepdims=True))


def rotary_tables(positions):
    half = HEAD_SIZE // 2
    freq = jnp.power(ROPE_THETA, -(2.0 * jnp.arange(half, dtype=F32)) / HEAD_SIZE)
    angle = positions[..., None] * freq
    return (jnp.cos(angle), jnp.sin(angle))


def rotary(values, cosine, sine):
    shape = values.shape
    heads = values.reshape(shape[:-1] + (shape[-1] // HEAD_SIZE, HEAD_SIZE))
    half = HEAD_SIZE // 2
    front = heads[..., :half]
    back = heads[..., half:]
    cos_h = cosine[..., None, :]
    sin_h = sine[..., None, :]
    return jnp.concatenate(
        [front * cos_h - back * sin_h, back * cos_h + front * sin_h], axis=-1
    ).reshape(shape)


def dot(left, right):
    return jnp.dot(left, right, preferred_element_type=F32)


def dot_nt(left, right):
    return lax.dot_general(left, right, (((1,), (1,)), ((), ())), preferred_element_type=F32)


def dot_tn(left, right):
    return lax.dot_general(left, right, (((0,), (0,)), ((), ())), preferred_element_type=F32)


def owner_bits(seq_size, dp_size):
    return (seq_size.bit_length() - 1, seq_size.bit_length() + dp_size.bit_length() - 2)


def my_bit(bit, seq_bits):
    if bit < seq_bits:
        return (lax.axis_index("seq") // 2**bit) % 2
    return (lax.axis_index("dp") // 2 ** (bit - seq_bits)) % 2


def partner_of(bit, seq_bits):
    axis, power = ("seq", 2**bit) if bit < seq_bits else ("dp", 2 ** (bit - seq_bits))
    return {axis: lax.axis_index(axis) + power * (1 - 2 * my_bit(bit, seq_bits))}


def exchange_kernel(count, bits, seq_bits, chunks, gather, *refs):
    sources, outs, refs = refs[:count], refs[count : 2 * count], refs[2 * count :]
    held = [refs[stage * count : (stage + 1) * count] for stage in range(bits)]
    refs = refs[bits * count :]
    if gather:
        whole, refs = refs[:count], refs[count:]
    send_sem, recv_sem, out_sem = refs
    every = list(range(bits - 1, -1, -1))
    core = min(seq_bits, bits - 1)
    rest = [bit for bit in every if bit != core]
    me = {bit: my_bit(bit, seq_bits) for bit in every}
    there = {bit: partner_of(bit, seq_bits) for bit in every}
    copies = []

    barrier = pltpu.get_barrier_semaphore()
    for bit in every:
        pl.semaphore_signal(
            barrier, inc=1, device_id=there[bit], device_id_type=pl.DeviceIdType.MESH
        )
    pl.semaphore_wait(barrier, bits)

    def order_of(number):
        turn = number % len(rest)
        return [core] + rest[turn:] + rest[:turn]

    def place(left, chosen, columns):
        return tuple(chosen.get(bit, slice(None)) for bit in left) + (slice(None), columns)

    def send(source, target, slot, number, bit):
        copy = pltpu.make_async_remote_copy(
            src_ref=source,
            dst_ref=target,
            send_sem=send_sem.at[slot, number],
            recv_sem=recv_sem.at[slot, number],
            device_id=there[bit],
            device_id_type=pl.DeviceIdType.MESH,
        )
        copy.start()
        copies.append(copy)
        return copy

    arriving = {}
    for number, (index, columns) in enumerate(chunks):
        left = list(every)
        source = sources[index].at[place(left, {core: 1 - me[core]}, columns)]
        left.remove(core)
        target = held[0][index].at[place(left, {}, columns)]
        arriving[number] = send(source, target, 0, number, core)

    def summed(number, stage, chosen):
        index, columns = chunks[number]
        order = order_of(number)
        known = dict(chosen)
        for bit in order[:stage]:
            known[bit] = me[bit]
        left = list(every)
        total = sources[index][place(left, known, columns)].astype(F32)
        for past in range(stage):
            left = [bit for bit in left if bit != order[past]]
            total = total + held[past][index][place(left, known, columns)].astype(F32)
        return total

    for stage in range(1, bits):
        for number, (index, columns) in enumerate(chunks):
            order = order_of(number)
            bit = order[stage]
            arriving[number].wait_recv()
            left = [b for b in every if b not in order[:stage]]
            spot = place(left, {bit: 1 - me[bit]}, columns)
            held[stage - 1][index][spot] = summed(number, stage, {bit: 1 - me[bit]}).astype(LOW)
            left.remove(bit)
            target = held[stage][index].at[place(left, {}, columns)]
            arriving[number] = send(held[stage - 1][index].at[spot], target, stage, number, bit)

    for number, (index, columns) in enumerate(chunks):
        arriving[number].wait_recv()
        total = summed(number, bits, {})
        if not gather:
            outs[index][:, columns] = total
            continue
        order = order_of(number)
        spot = place(every, me, columns)
        whole[index][spot] = total.astype(LOW)
        target = whole[index].at[spot]
        arriving[number] = send(target, target, bits, number, order[-1])

    if gather:
        for back in range(1, bits):
            for number, (index, columns) in enumerate(chunks):
                order = order_of(number)
                arriving[number].wait_recv()
                known = {bit: me[bit] for bit in order[: bits - back]}
                target = whole[index].at[place(every, known, columns)]
                arriving[number] = send(target, target, bits + back, number, order[bits - back - 1])
        for number in range(len(chunks)):
            arriving[number].wait_recv()
        for copy in copies:
            copy.wait_send()
        locals_ = [
            pltpu.make_async_copy(whole[index], outs[index], out_sem.at[index])
            for index in range(count)
        ]
        for copy in locals_:
            copy.start()
        for copy in locals_:
            copy.wait()
    else:
        for copy in copies:
            copy.wait_send()


def exchange(arrays, sizes, name, number, gather=False, chunk=512):
    seq_bits, bits = owner_bits(*sizes)
    parts = 2**bits
    views, chunks = [], []
    for index, array in enumerate(arrays):
        rows, columns = array.shape
        views.append(array.reshape((2,) * bits + (rows // parts, columns)))
        step = chunk if columns % chunk == 0 else columns
        for begin in range(0, columns, step):
            chunks.append((index, pl.ds(begin, step)))
    count = len(arrays)
    shapes = [view.shape[bits:] for view in views]
    scratch = [
        pltpu.VMEM((2,) * (bits - 1 - stage) + shape, LOW) for stage in range(bits) for shape in shapes
    ]
    slots = bits
    if gather:
        scratch += [pltpu.VMEM((2,) * bits + shape, LOW) for shape in shapes]
        slots = 2 * bits
        out_shape = [jax.ShapeDtypeStruct((2,) * bits + shape, LOW) for shape in shapes]
        out_specs = [pl.BlockSpec(memory_space=pl.ANY)] * count
    else:
        out_shape = [jax.ShapeDtypeStruct(shape, F32) for shape in shapes]
        out_specs = [pl.BlockSpec(memory_space=pltpu.VMEM)] * count
    scratch += [
        pltpu.SemaphoreType.DMA((slots, len(chunks))),
        pltpu.SemaphoreType.DMA((slots, len(chunks))),
        pltpu.SemaphoreType.DMA((count,)),
    ]
    moved = sum(view.size for view in views) * 2
    results = pl.pallas_call(
        functools.partial(exchange_kernel, count, bits, seq_bits, chunks, gather),
        out_shape=out_shape,
        in_specs=[pl.BlockSpec(memory_space=pltpu.VMEM)] * count,
        out_specs=out_specs,
        scratch_shapes=scratch,
        compiler_params=pltpu.CompilerParams(
            collective_id=number, has_side_effects=True, vmem_limit_bytes=48 * 2**20
        ),
        cost_estimate=pl.CostEstimate(flops=0, bytes_accessed=16 * moved, transcendentals=0),
        name=name,
    )(*views)
    if gather:
        results = [r.reshape(a.shape) for r, a in zip(results, arrays)]
    return results


def schulz_kernel(packed, tile, gram_ref, moment_ref, step_ref, gram, low_gram, poly, low_poly, low_mix):
    size = gram.shape[0]
    tiles = size // tile

    def rows(step):
        return pl.ds(pl.multiple_of(step * tile, tile), tile)

    if packed:
        half = size // 2
        gram[:half, :half] = gram_ref[0].astype(F32)
        gram[:half, half:] = gram_ref[1].astype(F32)
        gram[half:, :half] = gram_ref[1].astype(F32).T
        gram[half:, half:] = gram_ref[2].astype(F32)
    else:
        gram[...] = gram_ref[...].astype(F32)

    def diagonal(step, total):
        block = gram[rows(step), :]
        row = lax.broadcasted_iota(jnp.int32, block.shape, 0) + step * tile
        column = lax.broadcasted_iota(jnp.int32, block.shape, 1)
        return total + jnp.sum(
            jnp.sum(jnp.where(row == column, block, 0.0), axis=0, keepdims=True),
            axis=1,
            keepdims=True,
        )

    trace = lax.fori_loop(0, tiles, diagonal, jnp.zeros((1, 1), F32))
    inverse = 1.0 / (jnp.sqrt(trace) + EPS_MUON)
    square = inverse * inverse

    def scale(step, carry):
        block = gram[rows(step), :] * square
        gram[rows(step), :] = block
        low_gram[rows(step), :] = block.astype(LOW)
        return carry

    lax.fori_loop(0, tiles, scale, 0)
    ortho = moment_ref[...] * inverse
    for turn in range(ITERS_NS):

        def polynomial(step, carry):
            block = NS_B * gram[rows(step), :] + NS_C * dot(low_gram[rows(step), :], low_gram[...])
            poly[rows(step), :] = block
            low_poly[rows(step), :] = block.astype(LOW)
            return carry

        lax.fori_loop(0, tiles, polynomial, 0)
        ortho = NS_A * ortho + dot(ortho.astype(LOW), low_poly[...])
        if turn < ITERS_NS - 1:

            def mix(step, carry):
                block = (2.0 * NS_A) * poly[rows(step), :] + dot(low_poly[rows(step), :], low_poly[...])
                low_mix[rows(step), :] = block.astype(LOW)
                return carry

            lax.fori_loop(0, tiles, mix, 0)

            def advance(step, carry):
                block = (NS_A * NS_A) * gram[rows(step), :] + dot(low_gram[rows(step), :], low_mix[...])
                gram[rows(step), :] = block
                return carry

            lax.fori_loop(0, tiles, advance, 0)

            def lower(step, carry):
                low_gram[rows(step), :] = gram[rows(step), :].astype(LOW)
                return carry

            lax.fori_loop(0, tiles, lower, 0)
    step_ref[...] = (-LR_MUON * 0.2 * math.sqrt(MODEL_WIDTH)) * ortho


def newton_schulz(gram, moment, packed):
    size = moment.shape[1]
    tile = 256 if size % 256 == 0 else 128 if size % 128 == 0 else size
    big = (size, size)
    vmem = pl.BlockSpec(memory_space=pltpu.VMEM)
    flops = 2 * size * size * (7 * size + 3 * moment.shape[0])
    return pl.pallas_call(
        functools.partial(schulz_kernel, packed, tile),
        out_shape=jax.ShapeDtypeStruct(moment.shape, F32),
        in_specs=[vmem, vmem],
        out_specs=vmem,
        scratch_shapes=[
            pltpu.VMEM(big, F32),
            pltpu.VMEM(big, LOW),
            pltpu.VMEM(big, F32),
            pltpu.VMEM(big, LOW),
            pltpu.VMEM(big, LOW),
        ],
        compiler_params=pltpu.CompilerParams(vmem_limit_bytes=40 * 2**20),
        cost_estimate=pl.CostEstimate(flops=flops, bytes_accessed=3 * size * size, transcendentals=0),
        name="schulz",
    )(gram, moment)


def adam(grad, first, second):
    first_new = BETA_ONE * first + (1.0 - BETA_ONE) * grad
    second_new = BETA_TWO * second + (1.0 - BETA_TWO) * grad * grad
    corrected = first_new / (1.0 - BETA_ONE**ADAM_STEP)
    spread = jnp.sqrt(second_new / (1.0 - BETA_TWO**ADAM_STEP)) + EPS_ADAM
    return (first_new, second_new, -LR_ADAM * corrected / spread)


def shards(
    inputs,
    segment_ids,
    ancestry,
    w_query,
    key_weight,
    value_weight,
    w_output,
    w_gate,
    w_up,
    w_down,
    attn_gain,
    ffn_gain,
    cotangent,
    mom_query,
    key_momentum,
    value_momentum,
    mom_output,
    mom_gate,
    mom_up,
    mom_down,
    attn_first,
    attn_second,
    ffn_first,
    ffn_second,
):
    batches = inputs.shape[1]
    tokens = inputs.shape[2]
    tree_len = segment_ids.shape[2]
    seg_count = ancestry.shape[2]
    q_width = w_query.shape[1]
    kv_width = key_weight.shape[1]
    kv_heads = kv_width // HEAD_SIZE
    group = q_width // kv_width
    scale = 1.0 / math.sqrt(HEAD_SIZE)
    seq_size = tree_len // tokens
    inputs_share = w_gate.shape[0] // mom_gate.shape[0] // seq_size
    seq_me = lax.axis_index("seq")
    start = seq_me * tokens
    query_index = start + jnp.arange(tokens, dtype=jnp.int32)
    labels = jnp.arange(seg_count, dtype=jnp.int32)
    swap = [(0, 1), (1, 0)]
    if seq_size == 2:
        key_index = jnp.concatenate(
            [query_index, (1 - seq_me) * tokens + jnp.arange(tokens, dtype=jnp.int32)]
        )
    else:
        key_index = jnp.arange(tree_len, dtype=jnp.int32)

    def spread_keys(own):
        if seq_size == 2:
            return jnp.concatenate([own, lax.ppermute(own, "seq", swap)], axis=0)
        return lax.all_gather(own, "seq", axis=0, tiled=True)

    def collect_keys(grads):
        if seq_size == 2:
            other = lax.ppermute(grads[tokens:].astype(LOW), "seq", swap)
            return grads[:tokens] + other.astype(F32)
        return lax.psum_scatter(grads, "seq", scatter_dimension=0, tiled=True)

    queue = []

    def tensor_sum(partial):
        if queue:
            partial, queue[0] = lax.optimization_barrier((partial, queue[0]))
        total = lax.psum(partial, "tensor")
        queue[:] = [total]
        return total

    w_output_all = lax.all_gather(w_output, "tensor", axis=0, tiled=True)

    def stage_one(b):
        s = {}
        seg = segment_ids[0, b]
        member = (seg[:, None] == labels[None, :]).astype(F32)
        member_own = lax.dynamic_slice_in_dim(member, start, tokens, 0)
        if seq_size == 2:
            member_other = lax.dynamic_slice_in_dim(member, (1 - seq_me) * tokens, tokens, 0)
            member = jnp.concatenate([member_own, member_other], axis=0)
        reach = dot(member_own, ancestry[0, b].astype(F32))
        on_path = dot_nt(reach, member) > 0.5
        allowed = on_path & (query_index[:, None] >= key_index[None, :])
        positions = (jnp.sum(allowed.astype(jnp.int32), axis=1) - 1).astype(F32)
        s["allowed"] = allowed
        s["cos"], s["sin"] = rotary_tables(positions)
        resid = inputs[0, b].astype(F32)
        s["resid"] = resid
        s["scale_one"] = rms_scale(resid)
        s["plain_one"] = resid * s["scale_one"]
        s["normed_one"] = (s["plain_one"] * attn_gain).astype(LOW)
        s["query"] = rotary(dot(s["normed_one"], w_query), s["cos"], s["sin"]).astype(LOW)
        key = rotary(dot(s["normed_one"], key_weight), s["cos"], s["sin"]).astype(LOW)
        value = dot(s["normed_one"], value_weight).astype(LOW)
        s["kv"] = spread_keys(jnp.concatenate([key, value], axis=1))
        return s

    def scores_of(s):
        query_heads = s["query"].reshape(tokens, kv_heads, group, HEAD_SIZE)
        key_heads = s["kv"][:, :kv_width].reshape(tree_len, kv_heads, HEAD_SIZE)
        return (
            jnp.einsum("tkgd,skd->kgts", query_heads, key_heads, preferred_element_type=F32) * scale
        )

    def stage_two(s):
        masked = jnp.where(s["allowed"][None, None], scores_of(s), -1e30)
        top = jnp.max(masked, axis=-1, keepdims=True)
        expo = jnp.exp(masked - top)
        total = jnp.sum(expo, axis=-1, keepdims=True)
        s["logsum"] = top + jnp.log(total)
        probs = (expo / total).astype(LOW)
        value_heads = s["kv"][:, kv_width:].reshape(tree_len, kv_heads, HEAD_SIZE)
        s["mixed"] = (
            jnp.einsum("kgts,skd->tkgd", probs, value_heads, preferred_element_type=F32)
            .reshape(tokens, q_width)
            .astype(LOW)
        )
        s["mixed_all"] = lax.all_gather(s["mixed"], "tensor", axis=1, tiled=True)

    def stage_three(s, b):
        middle = s["resid"] + dot(s["mixed_all"], w_output_all)
        s["scale_two"] = rms_scale(middle)
        s["plain_two"] = middle * s["scale_two"]
        s["normed_two"] = (s["plain_two"] * ffn_gain).astype(LOW)
        gate = dot(s["normed_two"], w_gate)
        up_value = dot(s["normed_two"], w_up)
        sigma = jax.nn.sigmoid(gate)
        active = gate * sigma
        s["inner"] = (active * up_value).astype(LOW)
        block_cot = cotangent[0, b]
        inner_grad = dot_nt(block_cot, w_down)
        s["gate_grad"] = (inner_grad * up_value * sigma * (1.0 + gate * (1.0 - sigma))).astype(LOW)
        s["up_grad"] = (inner_grad * active).astype(LOW)
        two_partial = dot_nt(s["gate_grad"], w_gate) + dot_nt(s["up_grad"], w_up)
        s["two_sum"] = tensor_sum(two_partial.astype(LOW))
        s["middle"] = middle

    def stage_four(s, b):
        normed_two_grad = s["two_sum"].astype(F32)
        s["gain_two"] = jnp.sum(normed_two_grad * s["plain_two"], axis=0)
        s["middle_grad"] = cotangent[0, b].astype(F32) + norm_back(
            normed_two_grad, s["plain_two"], s["scale_two"], ffn_gain
        )
        s["middle_low"] = s["middle_grad"].astype(LOW)
        mixed_grad = dot_nt(s["middle_low"], w_output).astype(LOW)
        probs_full = jnp.exp(
            jnp.where(s["allowed"][None, None], scores_of(s), -1e30) - s["logsum"]
        )
        probs_low = probs_full.astype(LOW)
        mixed_heads = mixed_grad.reshape(tokens, kv_heads, group, HEAD_SIZE)
        value_heads = s["kv"][:, kv_width:].reshape(tree_len, kv_heads, HEAD_SIZE)
        key_heads = s["kv"][:, :kv_width].reshape(tree_len, kv_heads, HEAD_SIZE)
        query_heads = s["query"].reshape(tokens, kv_heads, group, HEAD_SIZE)
        prob_grad = jnp.einsum("tkgd,skd->kgts", mixed_heads, value_heads, preferred_element_type=F32)
        value_grad = jnp.einsum(
            "kgts,tkgd->skd", probs_low, mixed_heads, preferred_element_type=F32
        ).reshape(tree_len, kv_width)
        score_grad = (
            probs_full * (prob_grad - jnp.sum(probs_full * prob_grad, axis=-1, keepdims=True))
        ).astype(LOW)
        query_grad = (
            jnp.einsum("kgts,skd->tkgd", score_grad, key_heads, preferred_element_type=F32).reshape(
                tokens, q_width
            )
            * scale
        )
        key_grad = (
            jnp.einsum("kgts,tkgd->skd", score_grad, query_heads, preferred_element_type=F32).reshape(
                tree_len, kv_width
            )
            * scale
        )
        kv_grad = collect_keys(jnp.concatenate([key_grad, value_grad], axis=1))
        s["query_low"] = rotary(query_grad, s["cos"], -s["sin"]).astype(LOW)
        s["key_low"] = rotary(kv_grad[:, :kv_width], s["cos"], -s["sin"]).astype(LOW)
        s["value_low"] = kv_grad[:, kv_width:].astype(LOW)
        one_partial = (
            dot_nt(s["query_low"], w_query)
            + dot_nt(s["key_low"], key_weight)
            + dot_nt(s["value_low"], value_weight)
        )
        s["ffn_sum"] = tensor_sum(dot(s["inner"], w_down).astype(LOW))
        s["one_sum"] = tensor_sum(one_partial.astype(LOW))

    def stage_five(s):
        normed_one_grad = s["one_sum"].astype(F32)
        s["gain_one"] = jnp.sum(normed_one_grad * s["plain_one"], axis=0)
        s["block_out"] = s["middle"] + s["ffn_sum"].astype(F32)
        s["input_grad"] = s["middle_grad"] + norm_back(
            normed_one_grad, s["plain_one"], s["scale_one"], attn_gain
        )

    def weight_grad(lefts, rights):
        total = dot_tn(lefts[0], rights[0])
        for left, right in zip(lefts[1:], rights[1:]):
            total = total + dot_tn(left, right)
        return total.astype(LOW)

    def column(name):
        return [s[name] for s in states]

    sizes = (seq_size, inputs_share)

    def finish(grads, olds, name, number):
        sums = exchange(grads, sizes, name + "_grads", number)
        moments = [MU_MUON * old + total for old, total in zip(olds, sums)]
        return sums, moments

    def gram_of(moment):
        low = moment.astype(LOW)
        return dot_tn(low, low).astype(LOW)

    def packed_gram(moment):
        low = moment.astype(LOW)
        half = low.shape[1] // 2
        front, back = low[:, :half], low[:, half:]
        return [dot_tn(front, front), dot_tn(front, back), dot_tn(back, back)]

    states = [stage_one(b) for b in range(batches)]
    for s in states:
        stage_two(s)
    for b, s in enumerate(states):
        stage_three(s, b)
    cots = [cotangent[0, b] for b in range(batches)]
    ffn_grads = [
        weight_grad(column("normed_two"), column("gate_grad")),
        weight_grad(column("normed_two"), column("up_grad")),
        weight_grad(cots, column("inner")),
    ]
    for b, s in enumerate(states):
        stage_four(s, b)
    ffn_sums, ffn_moments = finish(ffn_grads, [mom_gate, mom_up, mom_down.T], "ffn", 0)
    half = ffn_moments[0].shape[1] // 2
    grams = jnp.concatenate(
        [jnp.concatenate(packed_gram(m), axis=0).astype(LOW) for m in ffn_moments], axis=1
    )
    (grams,) = exchange([grams], sizes, "ffn_grams", 1, gather=True)
    ffn_steps = [
        newton_schulz(
            grams[:, i * half : (i + 1) * half].reshape(3, half, half), ffn_moments[i], True
        )
        for i in range(3)
    ]
    attn_grads = [
        weight_grad(column("normed_one"), column("query_low")),
        weight_grad(column("normed_one"), column("key_low")),
        weight_grad(column("normed_one"), column("value_low")),
        weight_grad(column("middle_low"), column("mixed")),
    ]
    for s in states:
        stage_five(s)
    attn_sums, attn_moments = finish(
        attn_grads, [mom_query, key_momentum, value_momentum, mom_output.T], "attn", 2
    )
    pair = jnp.concatenate([gram_of(attn_moments[1]), gram_of(attn_moments[2])], axis=1)
    grams = jnp.concatenate([gram_of(attn_moments[0]), gram_of(attn_moments[3]), pair], axis=0)
    (grams,) = exchange([grams], sizes, "attn_grams", 3, gather=True)
    attn_steps = [
        newton_schulz(grams[:q_width], attn_moments[0], False),
        newton_schulz(grams[2 * q_width :, :kv_width], attn_moments[1], False),
        newton_schulz(grams[2 * q_width :, kv_width:], attn_moments[2], False),
        newton_schulz(grams[q_width : 2 * q_width], attn_moments[3], False),
    ]
    gains = jnp.stack([sum(column("gain_one")), sum(column("gain_two"))])
    gains = lax.psum(gains, ("dp", "seq"))
    attn_total, ffn_total = gains[0], gains[1]
    outputs = jnp.stack(column("block_out"))
    input_grads = jnp.stack(column("input_grad"))
    attn_one, attn_two, attn_step = adam(attn_total, attn_first, attn_second)
    ffn_one, ffn_two, ffn_step = adam(ffn_total, ffn_first, ffn_second)

    def listed(attn, ffn):
        return (attn[0], attn[1], attn[2], attn[3].T, ffn[0], ffn[1], ffn[2].T)

    return (
        (outputs[None], input_grads[None])
        + listed(attn_sums, ffn_sums)
        + (attn_total, ffn_total)
        + listed(attn_moments, ffn_moments)
        + listed(attn_steps, ffn_steps)
        + (attn_one, attn_two, attn_step, ffn_one, ffn_two, ffn_step)
    )


def solution(mesh):
    tokens = P("dp", None, "seq", None)
    column_split = P(None, "tensor")
    row_split = P("tensor", None)
    standing = P(("dp", "seq"), "tensor")
    lying = P("tensor", ("dp", "seq"))
    seven = (standing, standing, standing, lying, standing, standing, lying)
    placed = (
        (tokens, P("dp", None, None), P("dp", None, None, None))
        + (column_split, column_split, column_split, row_split)
        + (column_split, column_split, row_split)
        + (P(), P(), tokens)
        + seven
        + (P(), P(), P(), P())
    )
    results = (tokens, tokens) + seven + (P(), P()) + seven + seven + (P(),) * 6
    return jax.shard_map(shards, mesh=mesh, in_specs=placed, out_specs=results, check_vma=False)
```

```python
import functools
import math

import jax
import jax.numpy as jnp
from jax import lax
from jax.experimental import pallas as pl
from jax.experimental.pallas import tpu as pltpu
from jax.sharding import PartitionSpec as P

MODEL_WIDTH = 1536
HEAD_SIZE = 96
ITERS_NS = 3
ADAM_STEP = 10


EPS_NORM = 1e-05
ROPE_THETA = 100000.0
MU_MUON = 0.95
NS_A = 3.4445
NS_B = -4.775
NS_C = 2.0315
LR_MUON = 0.1
EPS_MUON = 1e-07
BETA_ONE = 0.9
BETA_TWO = 0.95
LR_ADAM = 0.01
EPS_ADAM = 1e-08
LOW = jnp.bfloat16
F32 = jnp.float32


def rms_scale(values):
    return lax.rsqrt(jnp.mean(values * values, axis=-1, keepdims=True) + EPS_NORM)


def norm_back(upstream, plain, scale, gain):
    scaled = upstream * gain
    return scale * (scaled - plain * jnp.mean(scaled * plain, axis=-1, keepdims=True))


def rotary_tables(positions):
    half = HEAD_SIZE // 2
    freq = jnp.power(ROPE_THETA, -(2.0 * jnp.arange(half, dtype=F32)) / HEAD_SIZE)
    angle = positions[..., None] * freq
    return (jnp.cos(angle), jnp.sin(angle))


def rotary(values, cosine, sine):
    shape = values.shape
    heads = values.reshape(shape[:-1] + (shape[-1] // HEAD_SIZE, HEAD_SIZE))
    half = HEAD_SIZE // 2
    front = heads[..., :half]
    back = heads[..., half:]
    cos_h = cosine[..., None, :]
    sin_h = sine[..., None, :]
    return jnp.concatenate(
        [front * cos_h - back * sin_h, back * cos_h + front * sin_h], axis=-1
    ).reshape(shape)


def dot(left, right):
    return jnp.dot(left, right, preferred_element_type=F32)


def dot_nt(left, right):
    return lax.dot_general(left, right, (((1,), (1,)), ((), ())), preferred_element_type=F32)


def dot_tn(left, right):
    return lax.dot_general(left, right, (((0,), (0,)), ((), ())), preferred_element_type=F32)


def owner_bits(seq_size, dp_size):
    return (seq_size.bit_length() - 1, seq_size.bit_length() + dp_size.bit_length() - 2)


def my_bit(bit, seq_bits):
    if bit < seq_bits:
        return (lax.axis_index("seq") // 2**bit) % 2
    return (lax.axis_index("dp") // 2 ** (bit - seq_bits)) % 2


def partner_of(bit, seq_bits):
    axis, power = ("seq", 2**bit) if bit < seq_bits else ("dp", 2 ** (bit - seq_bits))
    return {axis: lax.axis_index(axis) + power * (1 - 2 * my_bit(bit, seq_bits))}


def exchange_kernel(gathers, bits, seq_bits, chunks, lanes, pieces, lag, *refs):
    count, sums = len(gathers), 2 if pieces else 0
    sources, zin, refs = refs[:count], refs[count : count + sums], refs[count + sums :]
    outs, zout, refs = refs[:count], refs[count : count + sums], refs[count + sums :]
    held = [refs[stage * count : (stage + 1) * count] for stage in range(bits)]
    refs = refs[bits * count :]
    whole, refs = refs[:count], refs[count:]
    send_sem, recv_sem, out_sem = refs[:3]
    every = list(range(bits - 1, -1, -1))
    core = min(seq_bits, bits - 1)
    rest = [bit for bit in every if bit != core]
    me = {bit: my_bit(bit, seq_bits) for bit in every}
    there = {bit: partner_of(bit, seq_bits) for bit in every}
    copies = []
    mesh_ids = pl.DeviceIdType.MESH

    barrier = pltpu.get_barrier_semaphore()
    for bit in every:
        pl.semaphore_signal(barrier, inc=1, device_id=there[bit], device_id_type=mesh_ids)
    if sums:
        spot_z = lax.axis_index("tensor")
        for shift in (1, lanes - 1):
            pl.semaphore_signal(
                barrier,
                inc=1,
                device_id={"tensor": (spot_z + shift) % lanes},
                device_id_type=mesh_ids,
            )
    pl.semaphore_wait(barrier, bits + (2 if sums else 0))

    def order_of(number):
        turn = number % len(rest)
        return [core] + rest[turn:] + rest[:turn]

    def place(left, chosen, columns):
        return tuple(chosen.get(bit, slice(None)) for bit in left) + (slice(None), columns)

    def send(source, target, slot, number, bit):
        copy = pltpu.make_async_remote_copy(
            src_ref=source,
            dst_ref=target,
            send_sem=send_sem.at[slot, number],
            recv_sem=recv_sem.at[slot, number],
            device_id=there[bit],
            device_id_type=mesh_ids,
        )
        copy.start()
        copies.append(copy)
        return copy

    arriving = {}

    def halve_first(number):
        index, columns = chunks[number]
        left = list(every)
        source = sources[index].at[place(left, {core: 1 - me[core]}, columns)]
        left.remove(core)
        target = held[0][index].at[place(left, {}, columns)]
        arriving[number] = send(source, target, 0, number, core)

    def summed(number, stage, chosen):
        index, columns = chunks[number]
        order = order_of(number)
        known = dict(chosen)
        for bit in order[:stage]:
            known[bit] = me[bit]
        left = list(every)
        total = sources[index][place(left, known, columns)].astype(F32)
        for past in range(stage):
            left = [bit for bit in left if bit != order[past]]
            total = total + held[past][index][place(left, known, columns)].astype(F32)
        return total

    def halve(number, stage):
        index, columns = chunks[number]
        order = order_of(number)
        bit = order[stage]
        arriving[number].wait_recv()
        left = [b for b in every if b not in order[:stage]]
        spot = place(left, {bit: 1 - me[bit]}, columns)
        buffer = held[stage - 1][index]
        buffer[spot] = summed(number, stage, {bit: 1 - me[bit]}).astype(buffer.dtype)
        left.remove(bit)
        target = held[stage][index].at[place(left, {}, columns)]
        arriving[number] = send(buffer.at[spot], target, stage, number, bit)

    def settle(number):
        index, columns = chunks[number]
        arriving[number].wait_recv()
        total = summed(number, bits, {})
        if not gathers[index]:
            outs[index][:, columns] = total
            return
        spot = place(every, me, columns)
        whole[index][spot] = total.astype(whole[index].dtype)
        target = whole[index].at[spot]
        arriving[number] = send(target, target, bits, number, order_of(number)[-1])

    def double(number, back):
        index, columns = chunks[number]
        if not gathers[index]:
            return
        order = order_of(number)
        arriving[number].wait_recv()
        if back == bits:
            return
        known = {bit: me[bit] for bit in order[: bits - back]}
        target = whole[index].at[place(every, known, columns)]
        arriving[number] = send(target, target, bits + back, number, order[bits - back - 1])

    numbers = range(len(chunks))
    work = [functools.partial(halve, n, stage) for stage in range(1, bits) for n in numbers]
    work += [functools.partial(settle, n) for n in numbers]
    if any(gathers):
        work += [functools.partial(double, n, back) for back in range(1, bits + 1) for n in numbers]

    for number in numbers:
        halve_first(number)
    if sums:
        zacc, zsum, up_send, up_recv, back_send, back_recv, keep_sem = refs[3:]
        last = lanes - 1
        step = zin[0].shape[0] // pieces
        near = (2 * spot_z) // lanes
        far = 1 - near

        def chain(flow, piece):
            spot = spot_z + flow * (last - 2 * spot_z)
            ahead = {"tensor": (spot_z + lanes + 1 - 2 * flow) % lanes}
            behind = {"tensor": (spot_z + lanes - 1 + 2 * flow) % lanes}
            rows = pl.ds(piece * step, step)

            def up(source):
                return pltpu.make_async_remote_copy(
                    src_ref=source,
                    dst_ref=zacc.at[flow, rows],
                    send_sem=up_send.at[flow, piece],
                    recv_sem=up_recv.at[flow, piece],
                    device_id=ahead,
                    device_id_type=mesh_ids,
                )

            def back():
                return pltpu.make_async_remote_copy(
                    src_ref=zsum.at[flow, rows],
                    dst_ref=zsum.at[flow, rows],
                    send_sem=back_send.at[flow, piece],
                    recv_sem=back_recv.at[flow, piece],
                    device_id=behind,
                    device_id_type=mesh_ids,
                )

            return spot, rows, up, back

        def begin(flow, piece):
            spot, rows, up, back = chain(flow, piece)

            @pl.when(spot == 0)
            def _():
                up(zin[flow].at[rows]).start()

        def climb(flow, piece):
            spot, rows, up, back = chain(flow, piece)

            @pl.when(spot > 0)
            def _():
                up(zacc.at[flow, rows]).wait_recv()
                own = jnp.where(flow == 0, zin[0][rows, :].astype(F32), zin[1][rows, :].astype(F32))
                total = (own + zacc[flow, rows, :].astype(F32)).astype(LOW)

                @pl.when(spot < last)
                def _():
                    zacc[flow, rows, :] = total
                    up(zacc.at[flow, rows]).start()

                @pl.when(spot == last)
                def _():
                    zsum[flow, rows, :] = total
                    back().start()

        def descend(flow, piece):
            spot, rows, up, back = chain(flow, piece)

            @pl.when(spot < last)
            def _():
                back().wait_recv()

                @pl.when(spot > 0)
                def _():
                    back().start()

        def close(flow, piece):
            spot, rows, up, back = chain(flow, piece)

            @pl.when(spot < last)
            def _():
                up(zacc.at[flow, rows]).wait_send()

            @pl.when(spot > 0)
            def _():
                back().wait_send()

        for piece in range(pieces):
            for flow in range(2):
                begin(flow, piece)
        steps = []
        for work_of, first, second in ((climb, near, far), (descend, far, near)):
            for piece in range(pieces + lag):
                if piece < pieces:
                    steps.append(functools.partial(work_of, first, piece))
                if piece >= lag:
                    steps.append(functools.partial(work_of, second, piece - lag))
        done = 0
        for number, one in enumerate(steps):
            one()
            due = len(work) * max(0, number + 1 - len(steps) // 8) // (len(steps) - len(steps) // 8)
            for other in work[done:due]:
                other()
            done = due
        for piece in range(pieces):
            for flow in range(2):
                close(flow, piece)
    else:
        for one in work:
            one()
    for copy in copies:
        copy.wait_send()
    locals_ = [
        pltpu.make_async_copy(whole[index], outs[index], out_sem.at[index])
        for index in range(count)
        if gathers[index]
    ]
    if sums:
        locals_ += [
            pltpu.make_async_copy(zsum.at[flow], zout[flow], keep_sem.at[flow]) for flow in range(2)
        ]
    for copy in locals_:
        copy.start()
    for copy in locals_:
        copy.wait()


def exchange(arrays, gathers, sizes, name, number, partials=(), lanes=1, chunk=512, pieces=16, lag=2):
    seq_bits, bits = owner_bits(*sizes)
    parts = 2**bits
    views, chunks = [], []
    for index, array in enumerate(arrays):
        rows, columns = array.shape
        views.append(array.reshape((2,) * bits + (rows // parts, columns)))
        step = chunk if columns % chunk == 0 else columns
        for begin in range(0, columns, step):
            chunks.append((index, pl.ds(begin, step)))
    count = len(arrays)
    shapes = [view.shape[bits:] for view in views]
    kinds = [view.dtype for view in views]
    scratch = [
        pltpu.VMEM((2,) * (bits - 1 - stage) + shape, kind)
        for stage in range(bits)
        for shape, kind in zip(shapes, kinds)
    ]
    out_shape, out_specs = [], []
    for shape, kind, gather in zip(shapes, kinds, gathers):
        everywhere = (2,) * bits + shape
        scratch.append(pltpu.VMEM(everywhere if gather else (8, 128), kind))
        out_shape.append(jax.ShapeDtypeStruct(everywhere if gather else shape, kind if gather else F32))
        out_specs.append(pl.BlockSpec(memory_space=pl.ANY if gather else pltpu.VMEM))
    slots = (2 * bits if any(gathers) else bits, len(chunks))
    scratch += [
        pltpu.SemaphoreType.DMA(slots),
        pltpu.SemaphoreType.DMA(slots),
        pltpu.SemaphoreType.DMA((count,)),
    ]
    if partials:
        scratch += [pltpu.VMEM((2,) + partials[0].shape, partials[0].dtype)] * 2
        scratch += [pltpu.SemaphoreType.DMA((2, pieces)) for _ in range(4)]
        scratch.append(pltpu.SemaphoreType.DMA((2,)))
        out_shape += [jax.ShapeDtypeStruct(p.shape, p.dtype) for p in partials]
        out_specs += [pl.BlockSpec(memory_space=pl.ANY)] * 2
    moved = sum(view.size for view in views) * 2
    results = pl.pallas_call(
        functools.partial(
            exchange_kernel, gathers, bits, seq_bits, chunks, lanes, pieces if partials else 0, lag
        ),
        out_shape=out_shape,
        in_specs=[pl.BlockSpec(memory_space=pltpu.VMEM)] * (count + len(partials)),
        out_specs=out_specs,
        scratch_shapes=scratch,
        compiler_params=pltpu.CompilerParams(
            collective_id=number, has_side_effects=True, vmem_limit_bytes=48 * 2**20
        ),
        cost_estimate=pl.CostEstimate(flops=0, bytes_accessed=16 * moved, transcendentals=0),
        name=name,
    )(*views, *partials)
    sums = [
        r.reshape(a.shape) if gather else r for r, a, gather in zip(results, arrays, gathers)
    ]
    return sums, list(results[count:])


def schulz_kernel(packed, tile, gram_ref, moment_ref, step_ref, gram, low_gram, poly, low_poly, low_mix):
    size = gram.shape[0]
    tiles = size // tile

    def rows(step):
        return pl.ds(pl.multiple_of(step * tile, tile), tile)

    if packed:
        half = size // 2
        gram[:half, :half] = gram_ref[0].astype(F32)
        gram[:half, half:] = gram_ref[1].astype(F32)
        gram[half:, :half] = gram_ref[1].astype(F32).T
        gram[half:, half:] = gram_ref[2].astype(F32)
    else:
        gram[...] = gram_ref[...].astype(F32)

    def diagonal(step, total):
        block = gram[rows(step), :]
        row = lax.broadcasted_iota(jnp.int32, block.shape, 0) + step * tile
        column = lax.broadcasted_iota(jnp.int32, block.shape, 1)
        return total + jnp.sum(
            jnp.sum(jnp.where(row == column, block, 0.0), axis=0, keepdims=True),
            axis=1,
            keepdims=True,
        )

    trace = lax.fori_loop(0, tiles, diagonal, jnp.zeros((1, 1), F32))
    inverse = 1.0 / (jnp.sqrt(trace) + EPS_MUON)
    square = inverse * inverse

    def scale(step, carry):
        block = gram[rows(step), :] * square
        gram[rows(step), :] = block
        low_gram[rows(step), :] = block.astype(LOW)
        return carry

    lax.fori_loop(0, tiles, scale, 0)
    ortho = moment_ref[...] * inverse
    for turn in range(ITERS_NS):

        def polynomial(step, carry):
            block = NS_B * gram[rows(step), :] + NS_C * dot(low_gram[rows(step), :], low_gram[...])
            poly[rows(step), :] = block
            low_poly[rows(step), :] = block.astype(LOW)
            return carry

        lax.fori_loop(0, tiles, polynomial, 0)
        ortho = NS_A * ortho + dot(ortho.astype(LOW), low_poly[...])
        if turn < ITERS_NS - 1:

            def mix(step, carry):
                block = (2.0 * NS_A) * poly[rows(step), :] + dot(low_poly[rows(step), :], low_poly[...])
                low_mix[rows(step), :] = block.astype(LOW)
                return carry

            lax.fori_loop(0, tiles, mix, 0)

            def advance(step, carry):
                block = (NS_A * NS_A) * gram[rows(step), :] + dot(low_gram[rows(step), :], low_mix[...])
                gram[rows(step), :] = block
                return carry

            lax.fori_loop(0, tiles, advance, 0)

            def lower(step, carry):
                low_gram[rows(step), :] = gram[rows(step), :].astype(LOW)
                return carry

            lax.fori_loop(0, tiles, lower, 0)
    step_ref[...] = (-LR_MUON * 0.2 * math.sqrt(MODEL_WIDTH)) * ortho


def newton_schulz(gram, moment, packed):
    size = moment.shape[1]
    tile = 256 if size % 256 == 0 else 128 if size % 128 == 0 else size
    big = (size, size)
    vmem = pl.BlockSpec(memory_space=pltpu.VMEM)
    flops = 2 * size * size * (7 * size + 3 * moment.shape[0])
    return pl.pallas_call(
        functools.partial(schulz_kernel, packed, tile),
        out_shape=jax.ShapeDtypeStruct(moment.shape, F32),
        in_specs=[vmem, vmem],
        out_specs=vmem,
        scratch_shapes=[
            pltpu.VMEM(big, F32),
            pltpu.VMEM(big, LOW),
            pltpu.VMEM(big, F32),
            pltpu.VMEM(big, LOW),
            pltpu.VMEM(big, LOW),
        ],
        compiler_params=pltpu.CompilerParams(vmem_limit_bytes=40 * 2**20),
        cost_estimate=pl.CostEstimate(flops=flops, bytes_accessed=3 * size * size, transcendentals=0),
        name="schulz",
    )(gram, moment)


def adam(grad, first, second):
    first_new = BETA_ONE * first + (1.0 - BETA_ONE) * grad
    second_new = BETA_TWO * second + (1.0 - BETA_TWO) * grad * grad
    corrected = first_new / (1.0 - BETA_ONE**ADAM_STEP)
    spread = jnp.sqrt(second_new / (1.0 - BETA_TWO**ADAM_STEP)) + EPS_ADAM
    return (first_new, second_new, -LR_ADAM * corrected / spread)


def shards(
    inputs,
    segment_ids,
    ancestry,
    w_query,
    key_weight,
    value_weight,
    w_output,
    w_gate,
    w_up,
    w_down,
    attn_gain,
    ffn_gain,
    cotangent,
    mom_query,
    key_momentum,
    value_momentum,
    mom_output,
    mom_gate,
    mom_up,
    mom_down,
    attn_first,
    attn_second,
    ffn_first,
    ffn_second,
):
    batches = inputs.shape[1]
    tokens = inputs.shape[2]
    tree_len = segment_ids.shape[2]
    seg_count = ancestry.shape[2]
    q_width = w_query.shape[1]
    kv_width = key_weight.shape[1]
    kv_heads = kv_width // HEAD_SIZE
    group = q_width // kv_width
    scale = 1.0 / math.sqrt(HEAD_SIZE)
    seq_size = tree_len // tokens
    inputs_share = w_gate.shape[0] // mom_gate.shape[0] // seq_size
    seq_me = lax.axis_index("seq")
    start = seq_me * tokens
    query_index = start + jnp.arange(tokens, dtype=jnp.int32)
    labels = jnp.arange(seg_count, dtype=jnp.int32)
    swap = [(0, 1), (1, 0)]
    if seq_size == 2:
        key_index = jnp.concatenate(
            [query_index, (1 - seq_me) * tokens + jnp.arange(tokens, dtype=jnp.int32)]
        )
    else:
        key_index = jnp.arange(tree_len, dtype=jnp.int32)

    def spread_keys(own):
        if seq_size == 2:
            return jnp.concatenate([own, lax.ppermute(own, "seq", swap)], axis=0)
        return lax.all_gather(own, "seq", axis=0, tiled=True)

    def collect_keys(grads):
        if seq_size == 2:
            other = lax.ppermute(grads[tokens:].astype(LOW), "seq", swap)
            return grads[:tokens] + other.astype(F32)
        return lax.psum_scatter(grads, "seq", scatter_dimension=0, tiled=True)

    w_output_all = lax.all_gather(w_output, "tensor", axis=0, tiled=True)
    lanes = lax.axis_size("tensor")

    def after(value, earlier):
        return lax.optimization_barrier((value, earlier))[0]

    def stage_one(b):
        s = {}
        seg = segment_ids[0, b]
        member = (seg[:, None] == labels[None, :]).astype(F32)
        member_own = lax.dynamic_slice_in_dim(member, start, tokens, 0)
        if seq_size == 2:
            member_other = lax.dynamic_slice_in_dim(member, (1 - seq_me) * tokens, tokens, 0)
            member = jnp.concatenate([member_own, member_other], axis=0)
        reach = dot(member_own, ancestry[0, b].astype(F32))
        on_path = dot_nt(reach, member) > 0.5
        allowed = on_path & (query_index[:, None] >= key_index[None, :])
        positions = (jnp.sum(allowed.astype(jnp.int32), axis=1) - 1).astype(F32)
        s["allowed"] = allowed
        s["cos"], s["sin"] = rotary_tables(positions)
        resid = inputs[0, b].astype(F32)
        s["resid"] = resid
        s["scale_one"] = rms_scale(resid)
        s["plain_one"] = resid * s["scale_one"]
        s["normed_one"] = (s["plain_one"] * attn_gain).astype(LOW)
        s["query"] = rotary(dot(s["normed_one"], w_query), s["cos"], s["sin"]).astype(LOW)
        key = rotary(dot(s["normed_one"], key_weight), s["cos"], s["sin"]).astype(LOW)
        value = dot(s["normed_one"], value_weight).astype(LOW)
        s["kv"] = spread_keys(jnp.concatenate([key, value], axis=1))
        return s

    def scores_of(s):
        query_heads = s["query"].reshape(tokens, kv_heads, group, HEAD_SIZE)
        key_heads = s["kv"][:, :kv_width].reshape(tree_len, kv_heads, HEAD_SIZE)
        return (
            jnp.einsum("tkgd,skd->kgts", query_heads, key_heads, preferred_element_type=F32) * scale
        )

    def stage_two(s):
        masked = jnp.where(s["allowed"][None, None], scores_of(s), -1e30)
        top = jnp.max(masked, axis=-1, keepdims=True)
        expo = jnp.exp(masked - top)
        total = jnp.sum(expo, axis=-1, keepdims=True)
        s["logsum"] = top + jnp.log(total)
        probs = (expo / total).astype(LOW)
        value_heads = s["kv"][:, kv_width:].reshape(tree_len, kv_heads, HEAD_SIZE)
        s["mixed"] = (
            jnp.einsum("kgts,skd->tkgd", probs, value_heads, preferred_element_type=F32)
            .reshape(tokens, q_width)
            .astype(LOW)
        )
        s["mixed_all"] = lax.all_gather(
            after(s["mixed"], w_output_all), "tensor", axis=1, tiled=True
        )

    def stage_three(s, b):
        middle = s["resid"] + dot(s["mixed_all"], w_output_all)
        s["scale_two"] = rms_scale(middle)
        s["plain_two"] = middle * s["scale_two"]
        s["normed_two"] = (s["plain_two"] * ffn_gain).astype(LOW)
        gate = dot(s["normed_two"], w_gate)
        up_value = dot(s["normed_two"], w_up)
        sigma = jax.nn.sigmoid(gate)
        active = gate * sigma
        s["inner"] = (active * up_value).astype(LOW)
        block_cot = cotangent[0, b]
        inner_grad = dot_nt(block_cot, w_down)
        s["gate_grad"] = (inner_grad * up_value * sigma * (1.0 + gate * (1.0 - sigma))).astype(LOW)
        s["up_grad"] = (inner_grad * active).astype(LOW)
        two_partial = dot_nt(s["gate_grad"], w_gate) + dot_nt(s["up_grad"], w_up)
        s["two_partial"] = two_partial.astype(LOW)
        s["ffn_partial"] = dot(s["inner"], w_down).astype(LOW)
        s["middle"] = middle

    def stage_four(s, b):
        normed_two_grad = s["two_sum"].astype(F32)
        s["gain_two"] = jnp.sum(normed_two_grad * s["plain_two"], axis=0)
        s["middle_grad"] = cotangent[0, b].astype(F32) + norm_back(
            normed_two_grad, s["plain_two"], s["scale_two"], ffn_gain
        )
        s["middle_low"] = s["middle_grad"].astype(LOW)
        mixed_grad = dot_nt(s["middle_low"], w_output).astype(LOW)
        probs_full = jnp.exp(
            jnp.where(s["allowed"][None, None], scores_of(s), -1e30) - s["logsum"]
        )
        probs_low = probs_full.astype(LOW)
        mixed_heads = mixed_grad.reshape(tokens, kv_heads, group, HEAD_SIZE)
        value_heads = s["kv"][:, kv_width:].reshape(tree_len, kv_heads, HEAD_SIZE)
        key_heads = s["kv"][:, :kv_width].reshape(tree_len, kv_heads, HEAD_SIZE)
        query_heads = s["query"].reshape(tokens, kv_heads, group, HEAD_SIZE)
        prob_grad = jnp.einsum("tkgd,skd->kgts", mixed_heads, value_heads, preferred_element_type=F32)
        value_grad = jnp.einsum(
            "kgts,tkgd->skd", probs_low, mixed_heads, preferred_element_type=F32
        ).reshape(tree_len, kv_width)
        score_grad = (
            probs_full * (prob_grad - jnp.sum(probs_full * prob_grad, axis=-1, keepdims=True))
        ).astype(LOW)
        query_grad = (
            jnp.einsum("kgts,skd->tkgd", score_grad, key_heads, preferred_element_type=F32).reshape(
                tokens, q_width
            )
            * scale
        )
        key_grad = (
            jnp.einsum("kgts,tkgd->skd", score_grad, query_heads, preferred_element_type=F32).reshape(
                tree_len, kv_width
            )
            * scale
        )
        kv_grad = collect_keys(jnp.concatenate([key_grad, value_grad], axis=1))
        s["query_low"] = rotary(query_grad, s["cos"], -s["sin"]).astype(LOW)
        s["key_low"] = rotary(kv_grad[:, :kv_width], s["cos"], -s["sin"]).astype(LOW)
        s["value_low"] = kv_grad[:, kv_width:].astype(LOW)
        one_partial = (
            dot_nt(s["query_low"], w_query)
            + dot_nt(s["key_low"], key_weight)
            + dot_nt(s["value_low"], value_weight)
        )
        s["one_partial"] = one_partial.astype(LOW)

    def stage_five(s):
        normed_one_grad = s["one_sum"].astype(F32)
        s["gain_one"] = jnp.sum(normed_one_grad * s["plain_one"], axis=0)
        s["block_out"] = s["middle"] + s["ffn_sum"].astype(F32)
        s["input_grad"] = s["middle_grad"] + norm_back(
            normed_one_grad, s["plain_one"], s["scale_one"], attn_gain
        )

    def weight_grad(lefts, rights):
        total = dot_tn(lefts[0], rights[0])
        for left, right in zip(lefts[1:], rights[1:]):
            total = total + dot_tn(left, right)
        return total.astype(LOW)

    def column(name):
        return [s[name] for s in states]

    sizes = (seq_size, inputs_share)

    def momenta(olds, sums):
        return [MU_MUON * old + total for old, total in zip(olds, sums)]

    def gram_of(moment):
        low = moment.astype(LOW)
        return dot_tn(low, low).astype(LOW)

    def packed_gram(moment):
        low = moment.astype(LOW)
        half = low.shape[1] // 2
        front, back = low[:, :half], low[:, half:]
        return [dot_tn(front, front), dot_tn(front, back), dot_tn(back, back)]

    def tensor_pair(name):
        return [states[0][name], states[1][name]]

    states = [stage_one(b) for b in range(batches)]
    for s in states:
        stage_two(s)
    for b, s in enumerate(states):
        stage_three(s, b)
    cots = [cotangent[0, b] for b in range(batches)]
    ffn_grads = [
        weight_grad(column("normed_two"), column("gate_grad")),
        weight_grad(column("normed_two"), column("up_grad")),
        weight_grad(cots, column("inner")),
    ]
    ffn_sums, two_sums = exchange(
        ffn_grads, [False] * 3, sizes, "ffn_grads", 0, tensor_pair("two_partial"), lanes
    )
    for s, total in zip(states, two_sums):
        s["two_sum"] = total
    states[0]["ffn_sum"] = lax.psum(after(states[0]["ffn_partial"], two_sums[0]), "tensor")
    ffn_moments = momenta([mom_gate, mom_up, mom_down.T], ffn_sums)
    half = ffn_moments[0].shape[1] // 2
    grams = jnp.concatenate(
        [jnp.concatenate(packed_gram(m), axis=0).astype(LOW) for m in ffn_moments], axis=1
    )
    for b, s in enumerate(states):
        stage_four(s, b)
    attn_grads = [
        weight_grad(column("normed_one"), column("query_low")),
        weight_grad(column("normed_one"), column("key_low")),
        weight_grad(column("normed_one"), column("value_low")),
        weight_grad(column("middle_low"), column("mixed")),
    ]
    attn_sums, one_sums = exchange(
        [grams] + attn_grads,
        [True] + [False] * 4,
        sizes,
        "attn_grads",
        1,
        tensor_pair("one_partial"),
        lanes,
    )
    grams, attn_sums = attn_sums[0], attn_sums[1:]
    for s, total in zip(states, one_sums):
        s["one_sum"] = total
    states[1]["ffn_sum"] = lax.psum(
        after(states[1]["ffn_partial"], (states[0]["ffn_sum"], one_sums[0])), "tensor"
    )
    for s in states:
        stage_five(s)
    ffn_steps = [
        newton_schulz(
            grams[:, i * half : (i + 1) * half].reshape(3, half, half), ffn_moments[i], True
        )
        for i in range(3)
    ]
    attn_moments = momenta([mom_query, key_momentum, value_momentum, mom_output.T], attn_sums)
    pair = jnp.concatenate([gram_of(attn_moments[1]), gram_of(attn_moments[2])], axis=1)
    grams = jnp.concatenate([gram_of(attn_moments[0]), gram_of(attn_moments[3]), pair], axis=0)
    gains = jnp.stack([sum(column("gain_one")), sum(column("gain_two"))])
    owners = seq_size * inputs_share
    (grams, gains), _ = exchange(
        [grams, gains.reshape(owners, -1)], [True, True], sizes, "attn_grams", 2
    )
    gains = gains.reshape(2, -1)
    attn_total, ffn_total = gains[0], gains[1]
    attn_steps = [
        newton_schulz(grams[:q_width], attn_moments[0], False),
        newton_schulz(grams[2 * q_width :, :kv_width], attn_moments[1], False),
        newton_schulz(grams[2 * q_width :, kv_width:], attn_moments[2], False),
        newton_schulz(grams[q_width : 2 * q_width], attn_moments[3], False),
    ]
    outputs = jnp.stack(column("block_out"))
    input_grads = jnp.stack(column("input_grad"))
    attn_one, attn_two, attn_step = adam(attn_total, attn_first, attn_second)
    ffn_one, ffn_two, ffn_step = adam(ffn_total, ffn_first, ffn_second)

    def listed(attn, ffn):
        return (attn[0], attn[1], attn[2], attn[3].T, ffn[0], ffn[1], ffn[2].T)

    return (
        (outputs[None], input_grads[None])
        + listed(attn_sums, ffn_sums)
        + (attn_total, ffn_total)
        + listed(attn_moments, ffn_moments)
        + listed(attn_steps, ffn_steps)
        + (attn_one, attn_two, attn_step, ffn_one, ffn_two, ffn_step)
    )


def solution(mesh):
    tokens = P("dp", None, "seq", None)
    column_split = P(None, "tensor")
    row_split = P("tensor", None)
    standing = P(("dp", "seq"), "tensor")
    lying = P("tensor", ("dp", "seq"))
    seven = (standing, standing, standing, lying, standing, standing, lying)
    placed = (
        (tokens, P("dp", None, None), P("dp", None, None, None))
        + (column_split, column_split, column_split, row_split)
        + (column_split, column_split, row_split)
        + (P(), P(), tokens)
        + seven
        + (P(), P(), P(), P())
    )
    results = (tokens, tokens) + seven + (P(), P()) + seven + seven + (P(),) * 6
    return jax.shard_map(shards, mesh=mesh, in_specs=placed, out_specs=results, check_vma=False)
```

```python
import functools
import math

import jax
import jax.numpy as jnp
from jax import lax
from jax.experimental import pallas as pl
from jax.experimental.pallas import tpu as pltpu
from jax.sharding import PartitionSpec as P

MODEL_WIDTH = 1536
HEAD_SIZE = 96
ITERS_NS = 3
ADAM_STEP = 10


EPS_NORM = 1e-05
ROPE_THETA = 100000.0
MU_MUON = 0.95
NS_A = 3.4445
NS_B = -4.775
NS_C = 2.0315
LR_MUON = 0.1
EPS_MUON = 1e-07
BETA_ONE = 0.9
BETA_TWO = 0.95
LR_ADAM = 0.01
EPS_ADAM = 1e-08
LOW = jnp.bfloat16

F32 = jnp.float32


def rms_scale(values):
    return lax.rsqrt(jnp.mean(values * values, axis=-1, keepdims=True) + EPS_NORM)


def norm_back(upstream, plain, scale, gain):
    scaled = upstream * gain
    return scale * (scaled - plain * jnp.mean(scaled * plain, axis=-1, keepdims=True))


def rotary_tables(positions):
    half = HEAD_SIZE // 2
    freq = jnp.power(ROPE_THETA, -(2.0 * jnp.arange(half, dtype=F32)) / HEAD_SIZE)
    angle = positions[..., None] * freq
    return (jnp.cos(angle), jnp.sin(angle))


def rotary(values, cosine, sine):
    shape = values.shape
    heads = values.reshape(shape[:-1] + (shape[-1] // HEAD_SIZE, HEAD_SIZE))
    half = HEAD_SIZE // 2
    front = heads[..., :half]
    back = heads[..., half:]
    cos_h = cosine[..., None, :]
    sin_h = sine[..., None, :]
    return jnp.concatenate(
        [front * cos_h - back * sin_h, back * cos_h + front * sin_h], axis=-1
    ).reshape(shape)


def dot(left, right):
    return jnp.dot(left, right, preferred_element_type=F32)


def dot_nt(left, right):
    return lax.dot_general(left, right, (((1,), (1,)), ((), ())), preferred_element_type=F32)


def dot_tn(left, right):
    return lax.dot_general(left, right, (((0,), (0,)), ((), ())), preferred_element_type=F32)


def owner_bits(seq_size, dp_size):
    return (seq_size.bit_length() - 1, seq_size.bit_length() + dp_size.bit_length() - 2)


def my_bit(bit, seq_bits):
    if bit < seq_bits:
        return (lax.axis_index("seq") // 2**bit) % 2
    return (lax.axis_index("dp") // 2 ** (bit - seq_bits)) % 2


def partner_of(bit, seq_bits):
    axis, power = ("seq", 2**bit) if bit < seq_bits else ("dp", 2 ** (bit - seq_bits))
    return {axis: lax.axis_index(axis) + power * (1 - 2 * my_bit(bit, seq_bits))}


def exchange_kernel(gathers, bits, seq_bits, chunks, lanes, pieces, lag, carried, *refs):
    count, sums = len(gathers), 1 if pieces else 0
    sources, zin, refs = refs[:count], refs[count : count + sums], refs[count + sums + carried :]
    outs, zout, refs = refs[:count], refs[count : count + sums], refs[count + sums + carried :]
    held = [refs[stage * count : (stage + 1) * count] for stage in range(bits)]
    refs = refs[bits * count :]
    whole, refs = refs[:count], refs[count:]
    send_sem, recv_sem, out_sem = refs[:3]
    every = list(range(bits - 1, -1, -1))
    core = min(seq_bits, bits - 1)
    rest = [bit for bit in every if bit != core]
    me = {bit: my_bit(bit, seq_bits) for bit in every}
    there = {bit: partner_of(bit, seq_bits) for bit in every}
    copies = []
    mesh_ids = pl.DeviceIdType.MESH

    barrier = pltpu.get_barrier_semaphore()
    for bit in every:
        pl.semaphore_signal(barrier, inc=1, device_id=there[bit], device_id_type=mesh_ids)
    if sums:
        spot_z = lax.axis_index("tensor")
        for shift in (1, lanes - 1):
            pl.semaphore_signal(
                barrier,
                inc=1,
                device_id={"tensor": (spot_z + shift) % lanes},
                device_id_type=mesh_ids,
            )
    pl.semaphore_wait(barrier, bits + (2 if sums else 0))

    def order_of(number):
        turn = number % len(rest)
        return [core] + rest[turn:] + rest[:turn]

    def place(left, chosen, columns):
        return tuple(chosen.get(bit, slice(None)) for bit in left) + (slice(None), columns)

    def send(source, target, slot, number, bit):
        copy = pltpu.make_async_remote_copy(
            src_ref=source,
            dst_ref=target,
            send_sem=send_sem.at[slot, number],
            recv_sem=recv_sem.at[slot, number],
            device_id=there[bit],
            device_id_type=mesh_ids,
        )
        copy.start()
        copies.append(copy)
        return copy

    arriving = {}

    def halve_first(number):
        index, columns = chunks[number]
        left = list(every)
        source = sources[index].at[place(left, {core: 1 - me[core]}, columns)]
        left.remove(core)
        target = held[0][index].at[place(left, {}, columns)]
        arriving[number] = send(source, target, 0, number, core)

    def summed(number, stage, chosen):
        index, columns = chunks[number]
        order = order_of(number)
        known = dict(chosen)
        for bit in order[:stage]:
            known[bit] = me[bit]
        left = list(every)
        total = sources[index][place(left, known, columns)].astype(F32)
        for past in range(stage):
            left = [bit for bit in left if bit != order[past]]
            total = total + held[past][index][place(left, known, columns)].astype(F32)
        return total

    def halve(number, stage):
        index, columns = chunks[number]
        order = order_of(number)
        bit = order[stage]
        arriving[number].wait_recv()
        left = [b for b in every if b not in order[:stage]]
        spot = place(left, {bit: 1 - me[bit]}, columns)
        buffer = held[stage - 1][index]
        buffer[spot] = summed(number, stage, {bit: 1 - me[bit]}).astype(buffer.dtype)
        left.remove(bit)
        target = held[stage][index].at[place(left, {}, columns)]
        arriving[number] = send(buffer.at[spot], target, stage, number, bit)

    def settle(number):
        index, columns = chunks[number]
        arriving[number].wait_recv()
        total = summed(number, bits, {})
        if not gathers[index]:
            outs[index][:, columns] = total
            return
        spot = place(every, me, columns)
        whole[index][spot] = total.astype(whole[index].dtype)
        target = whole[index].at[spot]
        arriving[number] = send(target, target, bits, number, order_of(number)[-1])

    def double(number, back):
        index, columns = chunks[number]
        if not gathers[index]:
            return
        order = order_of(number)
        arriving[number].wait_recv()
        if back == bits:
            return
        known = {bit: me[bit] for bit in order[: bits - back]}
        target = whole[index].at[place(every, known, columns)]
        arriving[number] = send(target, target, bits + back, number, order[bits - back - 1])

    numbers = range(len(chunks))
    work = [functools.partial(halve, n, stage) for stage in range(1, bits) for n in numbers]
    work += [functools.partial(settle, n) for n in numbers]
    if any(gathers):
        work += [functools.partial(double, n, back) for back in range(1, bits + 1) for n in numbers]

    for number in numbers:
        halve_first(number)
    if sums:
        zacc, zsum, up_send, up_recv, back_send, back_recv, keep_sem = refs[3:]
        last = lanes - 1
        step = zin[0].shape[1] // pieces
        near = (2 * spot_z) // lanes
        far = 1 - near

        def chain(flow, piece):
            spot = spot_z + flow * (last - 2 * spot_z)
            ahead = {"tensor": (spot_z + lanes + 1 - 2 * flow) % lanes}
            behind = {"tensor": (spot_z + lanes - 1 + 2 * flow) % lanes}
            rows = pl.ds(piece * step, step)

            def up(source):
                return pltpu.make_async_remote_copy(
                    src_ref=source,
                    dst_ref=zacc.at[flow, rows],
                    send_sem=up_send.at[flow, piece],
                    recv_sem=up_recv.at[flow, piece],
                    device_id=ahead,
                    device_id_type=mesh_ids,
                )

            def back():
                return pltpu.make_async_remote_copy(
                    src_ref=zsum.at[flow, rows],
                    dst_ref=zsum.at[flow, rows],
                    send_sem=back_send.at[flow, piece],
                    recv_sem=back_recv.at[flow, piece],
                    device_id=behind,
                    device_id_type=mesh_ids,
                )

            return spot, rows, up, back

        def begin(flow, piece):
            spot, rows, up, back = chain(flow, piece)

            @pl.when(spot == 0)
            def _():
                up(zin[0].at[flow, rows]).start()

        def climb(flow, piece):
            spot, rows, up, back = chain(flow, piece)

            @pl.when(spot > 0)
            def _():
                up(zacc.at[flow, rows]).wait_recv()
                total = zin[0][flow, rows, :].astype(F32) + zacc[flow, rows, :].astype(F32)
                total = total.astype(LOW)

                @pl.when(spot < last)
                def _():
                    zacc[flow, rows, :] = total
                    up(zacc.at[flow, rows]).start()

                @pl.when(spot == last)
                def _():
                    zsum[flow, rows, :] = total
                    back().start()

        def descend(flow, piece):
            spot, rows, up, back = chain(flow, piece)

            @pl.when(spot < last)
            def _():
                back().wait_recv()

                @pl.when(spot > 0)
                def _():
                    back().start()

        def close(flow, piece):
            spot, rows, up, back = chain(flow, piece)

            @pl.when(spot < last)
            def _():
                up(zacc.at[flow, rows]).wait_send()

            @pl.when(spot > 0)
            def _():
                back().wait_send()

        for piece in range(pieces):
            for flow in range(2):
                begin(flow, piece)
        steps = []
        for work_of, first, second in ((climb, near, far), (descend, far, near)):
            for piece in range(pieces + lag):
                if piece < pieces:
                    steps.append(functools.partial(work_of, first, piece))
                if piece >= lag:
                    steps.append(functools.partial(work_of, second, piece - lag))
        done = 0
        for number, one in enumerate(steps):
            one()
            due = len(work) * max(0, number + 1 - len(steps) // 8) // (len(steps) - len(steps) // 8)
            for other in work[done:due]:
                other()
            done = due
        for piece in range(pieces):
            for flow in range(2):
                close(flow, piece)
    else:
        for one in work:
            one()
    for copy in copies:
        copy.wait_send()
    locals_ = [
        pltpu.make_async_copy(whole[index], outs[index], out_sem.at[index])
        for index in range(count)
        if gathers[index]
    ]
    if sums:
        locals_ += [
            pltpu.make_async_copy(zsum.at[flow], zout[0].at[flow], keep_sem.at[flow])
            for flow in range(2)
        ]
    for copy in locals_:
        copy.start()
    for copy in locals_:
        copy.wait()


def exchange(arrays, gathers, sizes, name, number, partial=None, lanes=1, carry=(), chunk=512, pieces=16, lag=2):
    seq_bits, bits = owner_bits(*sizes)
    parts = 2**bits
    views, chunks = [], []
    for index, array in enumerate(arrays):
        rows, columns = array.shape
        views.append(array.reshape((2,) * bits + (rows // parts, columns)))
        step = chunk if columns % chunk == 0 else columns
        for begin in range(0, columns, step):
            chunks.append((index, pl.ds(begin, step)))
    count = len(arrays)
    shapes = [view.shape[bits:] for view in views]
    kinds = [view.dtype for view in views]
    scratch = [
        pltpu.VMEM((2,) * (bits - 1 - stage) + shape, kind)
        for stage in range(bits)
        for shape, kind in zip(shapes, kinds)
    ]
    out_shape, out_specs = [], []
    for shape, kind, gather in zip(shapes, kinds, gathers):
        everywhere = (2,) * bits + shape
        scratch.append(pltpu.VMEM(everywhere if gather else (8, 128), kind))
        out_shape.append(jax.ShapeDtypeStruct(everywhere if gather else shape, kind if gather else F32))
        out_specs.append(pl.BlockSpec(memory_space=pl.ANY if gather else pltpu.VMEM))
    slots = (2 * bits if any(gathers) else bits, len(chunks))
    scratch += [
        pltpu.SemaphoreType.DMA(slots),
        pltpu.SemaphoreType.DMA(slots),
        pltpu.SemaphoreType.DMA((count,)),
    ]
    partials = []
    if partial is not None:
        partials = [partial.reshape(2, partial.shape[0] // 2, partial.shape[1])]
        scratch += [pltpu.VMEM(partials[0].shape, partial.dtype)] * 2
        scratch += [pltpu.SemaphoreType.DMA((2, pieces)) for _ in range(4)]
        scratch.append(pltpu.SemaphoreType.DMA((2,)))
        out_shape.append(jax.ShapeDtypeStruct(partials[0].shape, partial.dtype))
        out_specs.append(pl.BlockSpec(memory_space=pl.ANY))
    first_carried = count + len(partials)
    out_shape += [jax.ShapeDtypeStruct(c.shape, c.dtype) for c in carry]
    out_specs += [pl.BlockSpec(memory_space=pl.ANY)] * len(carry)
    moved = sum(view.size for view in views) * 2
    results = pl.pallas_call(
        functools.partial(
            exchange_kernel, gathers, bits, seq_bits, chunks, lanes, pieces if partials else 0, lag, len(carry)
        ),
        out_shape=out_shape,
        in_specs=[pl.BlockSpec(memory_space=pltpu.VMEM)] * first_carried
        + [pl.BlockSpec(memory_space=pl.ANY)] * len(carry),
        input_output_aliases={first_carried + i: first_carried + i for i in range(len(carry))},
        out_specs=out_specs,
        scratch_shapes=scratch,
        compiler_params=pltpu.CompilerParams(
            collective_id=number, has_side_effects=True, vmem_limit_bytes=48 * 2**20
        ),
        cost_estimate=pl.CostEstimate(flops=0, bytes_accessed=16 * moved, transcendentals=0),
        name=name,
    )(*views, *partials, *carry)
    sums = [
        r.reshape(a.shape) if gather else r for r, a, gather in zip(results, arrays, gathers)
    ]
    total = results[count].reshape(partial.shape) if partials else None
    return sums, total, list(results[first_carried:])


def schulz_kernel(packed, tile, gram_ref, moment_ref, step_ref, gram, low_gram, poly, low_poly, low_mix):
    size = gram.shape[0]
    tiles = size // tile

    def rows(step):
        return pl.ds(pl.multiple_of(step * tile, tile), tile)

    if packed:
        half = size // 2
        gram[:half, :half] = gram_ref[0].astype(F32)
        gram[:half, half:] = gram_ref[1].astype(F32)
        gram[half:, :half] = gram_ref[1].astype(F32).T
        gram[half:, half:] = gram_ref[2].astype(F32)
    else:
        gram[...] = gram_ref[...].astype(F32)

    def diagonal(step, total):
        block = gram[rows(step), :]
        row = lax.broadcasted_iota(jnp.int32, block.shape, 0) + step * tile
        column = lax.broadcasted_iota(jnp.int32, block.shape, 1)
        return total + jnp.sum(
            jnp.sum(jnp.where(row == column, block, 0.0), axis=0, keepdims=True),
            axis=1,
            keepdims=True,
        )

    trace = lax.fori_loop(0, tiles, diagonal, jnp.zeros((1, 1), F32))
    inverse = 1.0 / (jnp.sqrt(trace) + EPS_MUON)
    square = inverse * inverse

    def scale(step, carry):
        block = gram[rows(step), :] * square
        gram[rows(step), :] = block
        low_gram[rows(step), :] = block.astype(LOW)
        return carry

    lax.fori_loop(0, tiles, scale, 0)
    ortho = moment_ref[...] * inverse
    for turn in range(ITERS_NS):

        def polynomial(step, carry):
            block = NS_B * gram[rows(step), :] + NS_C * dot(low_gram[rows(step), :], low_gram[...])
            poly[rows(step), :] = block
            low_poly[rows(step), :] = block.astype(LOW)
            return carry

        lax.fori_loop(0, tiles, polynomial, 0)
        ortho = NS_A * ortho + dot(ortho.astype(LOW), low_poly[...])
        if turn < ITERS_NS - 1:

            def mix(step, carry):
                block = (2.0 * NS_A) * poly[rows(step), :] + dot(low_poly[rows(step), :], low_poly[...])
                low_mix[rows(step), :] = block.astype(LOW)
                return carry

            lax.fori_loop(0, tiles, mix, 0)

            def advance(step, carry):
                block = (NS_A * NS_A) * gram[rows(step), :] + dot(low_gram[rows(step), :], low_mix[...])
                gram[rows(step), :] = block
                return carry

            lax.fori_loop(0, tiles, advance, 0)

            def lower(step, carry):
                low_gram[rows(step), :] = gram[rows(step), :].astype(LOW)
                return carry

            lax.fori_loop(0, tiles, lower, 0)
    step_ref[...] = (-LR_MUON * 0.2 * math.sqrt(MODEL_WIDTH)) * ortho


def newton_schulz(gram, moment, packed):
    size = moment.shape[1]
    tile = 256 if size % 256 == 0 else size
    big = (size, size)
    vmem = pl.BlockSpec(memory_space=pltpu.VMEM)
    flops = 2 * size * size * (7 * size + 3 * moment.shape[0])
    return pl.pallas_call(
        functools.partial(schulz_kernel, packed, tile),
        out_shape=jax.ShapeDtypeStruct(moment.shape, F32),
        in_specs=[vmem, vmem],
        out_specs=vmem,
        scratch_shapes=[
            pltpu.VMEM(big, F32),
            pltpu.VMEM(big, LOW),
            pltpu.VMEM(big, F32),
            pltpu.VMEM(big, LOW),
            pltpu.VMEM(big, LOW),
        ],
        compiler_params=pltpu.CompilerParams(vmem_limit_bytes=40 * 2**20),
        cost_estimate=pl.CostEstimate(flops=flops, bytes_accessed=3 * size * size, transcendentals=0),
        name="schulz",
    )(gram, moment)


def adam(grad, first, second):
    first_new = BETA_ONE * first + (1.0 - BETA_ONE) * grad
    second_new = BETA_TWO * second + (1.0 - BETA_TWO) * grad * grad
    corrected = first_new / (1.0 - BETA_ONE**ADAM_STEP)
    spread = jnp.sqrt(second_new / (1.0 - BETA_TWO**ADAM_STEP)) + EPS_ADAM
    return (first_new, second_new, -LR_ADAM * corrected / spread)


def shards(
    inputs,
    segment_ids,
    ancestry,
    w_query,
    key_weight,
    value_weight,
    w_output,
    w_gate,
    w_up,
    w_down,
    attn_gain,
    ffn_gain,
    cotangent,
    mom_query,
    key_momentum,
    value_momentum,
    mom_output,
    mom_gate,
    mom_up,
    mom_down,
    attn_first,
    attn_second,
    ffn_first,
    ffn_second,
):
    batches = inputs.shape[1]
    tokens = inputs.shape[2]
    tree_len = segment_ids.shape[2]
    seg_count = ancestry.shape[2]
    width = inputs.shape[3]
    q_width = w_query.shape[1]
    kv_width = key_weight.shape[1]
    kv_heads = kv_width // HEAD_SIZE
    group = q_width // kv_width
    scale = 1.0 / math.sqrt(HEAD_SIZE)
    seq_size = tree_len // tokens
    owners = width // mom_gate.shape[0]
    sizes = (seq_size, owners // seq_size)
    lanes = lax.axis_size("tensor")
    seq_me = lax.axis_index("seq")
    start = seq_me * tokens
    query_index = start + jnp.arange(tokens, dtype=jnp.int32)
    labels = jnp.arange(seg_count, dtype=jnp.int32)
    swap = [(0, 1), (1, 0)]
    if seq_size == 2:
        key_index = jnp.concatenate(
            [query_index, (1 - seq_me) * tokens + jnp.arange(tokens, dtype=jnp.int32)]
        )
    else:
        key_index = jnp.arange(tree_len, dtype=jnp.int32)

    def spread_keys(own):
        if seq_size == 2:
            return jnp.concatenate([own, lax.ppermute(own, "seq", swap)], axis=0)
        return lax.all_gather(own, "seq", axis=0, tiled=True)

    def collect_keys(grads):
        if seq_size == 2:
            other = lax.ppermute(grads[tokens:].astype(LOW), "seq", swap)
            return grads[:tokens] + other.astype(F32)
        return lax.psum_scatter(grads, "seq", scatter_dimension=0, tiled=True)

    def gather_output_weights():
        share = q_width // owners
        if share % 16 or owners != 8:
            return lax.all_gather(w_output, "tensor", axis=0, tiled=True)
        axes = ("dp", "seq")
        lane = lax.axis_index("tensor")
        mine = lax.axis_index("dp") * seq_size + seq_me
        part = lax.dynamic_slice_in_dim(w_output, mine * share, share, 0)
        first = jnp.zeros((lanes, share, width), LOW)
        first = lax.dynamic_update_slice(first, part[None], (lane, 0, 0))
        for shift in range(1, lanes):
            pairs = [(index, (index + shift) % lanes) for index in range(lanes)]
            other = lax.ppermute(part, "tensor", pairs)
            first = lax.dynamic_update_slice(
                first, other[None], ((lane + lanes - shift) % lanes, 0, 0)
            )
        parts = {0: first}
        for flip in (1, 4, 2):
            pairs = [(index, index ^ flip) for index in range(owners)]
            for known in list(parts):
                parts[known ^ flip] = lax.ppermute(parts[known], axes, pairs)
        whole = jnp.zeros((lanes, owners, share, width), LOW)
        for flip, one in parts.items():
            whole = lax.dynamic_update_slice(whole, one[:, None], (0, mine ^ flip, 0, 0))
        return whole.reshape(lanes * q_width, width)

    def momenta(olds, sums):
        return [MU_MUON * old + total for old, total in zip(olds, sums)]

    def gram_of(moment):
        low = moment.astype(LOW)
        return dot_tn(low, low).astype(LOW)

    def packed_gram(moment):
        low = moment.astype(LOW)
        half = low.shape[1] // 2
        front, back = low[:, :half], low[:, half:]
        return [dot_tn(front, front), dot_tn(front, back), dot_tn(back, back)]

    def trees(array):
        return [array[b * tokens : (b + 1) * tokens] for b in range(batches)]

    every = batches * tokens
    w_output_all = gather_output_weights()

    allowed, positions = [], []
    for b in range(batches):
        member = (segment_ids[0, b][:, None] == labels[None, :]).astype(F32)
        member_own = lax.dynamic_slice_in_dim(member, start, tokens, 0)
        if seq_size == 2:
            member_other = lax.dynamic_slice_in_dim(member, (1 - seq_me) * tokens, tokens, 0)
            member = jnp.concatenate([member_own, member_other], axis=0)
        reach = dot(member_own, ancestry[0, b].astype(F32))
        on_path = dot_nt(reach, member) > 0.5
        allowed.append(on_path & (query_index[:, None] >= key_index[None, :]))
        positions.append((jnp.sum(allowed[b].astype(jnp.int32), axis=1) - 1).astype(F32))
    cosine, sine = rotary_tables(jnp.concatenate(positions))

    resid = inputs[0].reshape(every, width).astype(F32)
    scale_one = rms_scale(resid)
    plain_one = resid * scale_one
    normed_one = (plain_one * attn_gain).astype(LOW)
    key = rotary(dot(normed_one, key_weight), cosine, sine).astype(LOW)
    value = dot(normed_one, value_weight).astype(LOW)
    key_values = [spread_keys(kv) for kv in trees(jnp.concatenate([key, value], axis=1))]
    query = rotary(dot(normed_one, w_query), cosine, sine).astype(LOW)
    query_heads = [q.reshape(tokens, kv_heads, group, HEAD_SIZE) for q in trees(query)]
    key_heads = [kv[:, :kv_width].reshape(tree_len, kv_heads, HEAD_SIZE) for kv in key_values]
    value_heads = [kv[:, kv_width:].reshape(tree_len, kv_heads, HEAD_SIZE) for kv in key_values]

    def scores_of(b):
        scores = jnp.einsum(
            "tkgd,skd->kgts", query_heads[b], key_heads[b], preferred_element_type=F32
        )
        return jnp.where(allowed[b][None, None], scores * scale, -1e30)

    logsum, mixed = [], []
    for b in range(batches):
        masked = scores_of(b)
        top = jnp.max(masked, axis=-1, keepdims=True)
        expo = jnp.exp(masked - top)
        total = jnp.sum(expo, axis=-1, keepdims=True)
        logsum.append(top + jnp.log(total))
        probs = (expo / total).astype(LOW)
        mixed.append(
            jnp.einsum("kgts,skd->tkgd", probs, value_heads[b], preferred_element_type=F32)
            .reshape(tokens, q_width)
            .astype(LOW)
        )
    mixed = jnp.concatenate(mixed, axis=0)
    mixed_all = lax.all_gather(mixed, "tensor", axis=1, tiled=True)
    middle = resid + dot(mixed_all, w_output_all)

    cot = cotangent[0].reshape(every, width)
    scale_two = rms_scale(middle)
    plain_two = middle * scale_two
    normed_two = (plain_two * ffn_gain).astype(LOW)
    gate = dot(normed_two, w_gate)
    up_value = dot(normed_two, w_up)
    sigma = jax.nn.sigmoid(gate)
    active = gate * sigma
    inner = (active * up_value).astype(LOW)
    inner_grad = dot_nt(cot, w_down)
    gate_grad = (inner_grad * up_value * sigma * (1.0 + gate * (1.0 - sigma))).astype(LOW)
    up_grad = (inner_grad * active).astype(LOW)
    two_partial = (dot_nt(gate_grad, w_gate) + dot_nt(up_grad, w_up)).astype(LOW)
    ffn_grads = [
        dot_tn(normed_two, gate_grad).astype(LOW),
        dot_tn(normed_two, up_grad).astype(LOW),
        dot_tn(cot, inner).astype(LOW),
    ]
    middle_row = every // 2
    ffn_front, ffn_back = dot(inner[:middle_row], w_down), dot(inner[middle_row:], w_down)
    ffn_sums, two_sum, (ffn_front,) = exchange(
        ffn_grads, [False] * 3, sizes, "ffn_grads", 0, two_partial, lanes, [ffn_front.astype(LOW)]
    )
    ffn_front = lax.psum(ffn_front, "tensor")
    ffn_moments = momenta([mom_gate, mom_up, mom_down.T], ffn_sums)
    half = ffn_moments[0].shape[1] // 2
    grams = jnp.concatenate(
        [jnp.concatenate(packed_gram(m), axis=0).astype(LOW) for m in ffn_moments], axis=1
    )

    normed_two_grad = two_sum.astype(F32)
    gain_two = jnp.sum(normed_two_grad * plain_two, axis=0)
    middle_grad = cot.astype(F32) + norm_back(normed_two_grad, plain_two, scale_two, ffn_gain)
    middle_low = middle_grad.astype(LOW)
    mixed_grad = dot_nt(middle_low, w_output).astype(LOW)
    query_grad, kv_grad = [], []
    for b, mixed_heads in enumerate(trees(mixed_grad)):
        mixed_heads = mixed_heads.reshape(tokens, kv_heads, group, HEAD_SIZE)
        probs = jnp.exp(scores_of(b) - logsum[b])
        prob_grad = jnp.einsum(
            "tkgd,skd->kgts", mixed_heads, value_heads[b], preferred_element_type=F32
        )
        value_grad = jnp.einsum(
            "kgts,tkgd->skd", probs.astype(LOW), mixed_heads, preferred_element_type=F32
        ).reshape(tree_len, kv_width)
        score_grad = (
            probs * (prob_grad - jnp.sum(probs * prob_grad, axis=-1, keepdims=True))
        ).astype(LOW)
        query_grad.append(
            jnp.einsum("kgts,skd->tkgd", score_grad, key_heads[b], preferred_element_type=F32)
            .reshape(tokens, q_width)
            * scale
        )
        key_grad = (
            jnp.einsum("kgts,tkgd->skd", score_grad, query_heads[b], preferred_element_type=F32)
            .reshape(tree_len, kv_width)
            * scale
        )
        kv_grad.append(collect_keys(jnp.concatenate([key_grad, value_grad], axis=1)))
    query_low = rotary(jnp.concatenate(query_grad), cosine, -sine).astype(LOW)
    kv_grad = jnp.concatenate(kv_grad)
    key_low = rotary(kv_grad[:, :kv_width], cosine, -sine).astype(LOW)
    value_low = kv_grad[:, kv_width:].astype(LOW)
    one_partial = (
        dot_nt(query_low, w_query) + dot_nt(key_low, key_weight) + dot_nt(value_low, value_weight)
    ).astype(LOW)
    attn_grads = [
        dot_tn(normed_one, query_low).astype(LOW),
        dot_tn(normed_one, key_low).astype(LOW),
        dot_tn(normed_one, value_low).astype(LOW),
        dot_tn(middle_low, mixed).astype(LOW),
    ]
    attn_sums, one_sum, (ffn_front, ffn_back) = exchange(
        [grams] + attn_grads,
        [True] + [False] * 4,
        sizes,
        "attn_grads",
        1,
        one_partial,
        lanes,
        [ffn_front, ffn_back.astype(LOW)],
    )
    ffn_back = lax.psum(ffn_back, "tensor")
    grams, attn_sums = attn_sums[0], attn_sums[1:]

    normed_one_grad = one_sum.astype(F32)
    gain_one = jnp.sum(normed_one_grad * plain_one, axis=0)
    ffn_steps = [
        newton_schulz(
            grams[:, i * half : (i + 1) * half].reshape(3, half, half), ffn_moments[i], True
        )
        for i in range(3)
    ]
    attn_moments = momenta([mom_query, key_momentum, value_momentum, mom_output.T], attn_sums)
    pair = jnp.concatenate([gram_of(attn_moments[1]), gram_of(attn_moments[2])], axis=1)
    grams = jnp.concatenate([gram_of(attn_moments[0]), gram_of(attn_moments[3]), pair], axis=0)
    gains = jnp.stack([gain_one, gain_two]).reshape(owners, -1)
    (grams, gains), _, (ffn_back,) = exchange(
        [grams, gains], [True, True], sizes, "attn_grams", 2, carry=[ffn_back]
    )
    gains = gains.reshape(2, -1)
    attn_total, ffn_total = gains[0], gains[1]
    attn_steps = [
        newton_schulz(grams[:q_width], attn_moments[0], False),
        newton_schulz(grams[2 * q_width :, :kv_width], attn_moments[1], False),
        newton_schulz(grams[2 * q_width :, kv_width:], attn_moments[2], False),
        newton_schulz(grams[q_width : 2 * q_width], attn_moments[3], False),
    ]
    block_out = middle + jnp.concatenate([ffn_front, ffn_back]).astype(F32)
    input_grad = middle_grad + norm_back(normed_one_grad, plain_one, scale_one, attn_gain)
    outputs = block_out.reshape(batches, tokens, width)
    input_grads = input_grad.reshape(batches, tokens, width)
    attn_one, attn_two, attn_step = adam(attn_total, attn_first, attn_second)
    ffn_one, ffn_two, ffn_step = adam(ffn_total, ffn_first, ffn_second)

    def listed(attn, ffn):
        return (attn[0], attn[1], attn[2], attn[3].T, ffn[0], ffn[1], ffn[2].T)

    return (
        (outputs[None], input_grads[None])
        + listed(attn_sums, ffn_sums)
        + (attn_total, ffn_total)
        + listed(attn_moments, ffn_moments)
        + listed(attn_steps, ffn_steps)
        + (attn_one, attn_two, attn_step, ffn_one, ffn_two, ffn_step)
    )


def solution(mesh):
    tokens = P("dp", None, "seq", None)
    column_split = P(None, "tensor")
    row_split = P("tensor", None)
    standing = P(("dp", "seq"), "tensor")
    lying = P("tensor", ("dp", "seq"))
    seven = (standing, standing, standing, lying, standing, standing, lying)
    placed = (
        (tokens, P("dp", None, None), P("dp", None, None, None))
        + (column_split, column_split, column_split, row_split)
        + (column_split, column_split, row_split)
        + (P(), P(), tokens)
        + seven
        + (P(), P(), P(), P())
    )
    results = (tokens, tokens) + seven + (P(), P()) + seven + seven + (P(),) * 6
    return jax.shard_map(shards, mesh=mesh, in_specs=placed, out_specs=results, check_vma=False)
```
